32 devices in a mesh: dp: 8 (over z, y), mp: 4 (over x, core).
Axes of the slice: x: 2, y: 2, z: 4, core: 2. Of those that a mesh axis runs over, the one named last changes fastest.
Arguments:
- tokens: bfloat16 [6144, 768], P(('dp', 'mp')), may hold values from -6 to 6
- obs_mask: int32 [96, 64], P(('dp', 'mp')), may hold values 0 or 1
- norm_gains: float32 [5, 768], replicated, may hold values from 0.1 to 1.9
- attn_in: bfloat16 [2, 3, 768, 768], P(None, None, 'dp', 'mp'), may hold values from -0.21875 to 0.21875
- attn_out: bfloat16 [2, 768, 768], P(None, 'mp', 'dp'), may hold values from -0.21875 to 0.21875
- mlp_in: bfloat16 [2, 768, 3072], P(None, 'dp', 'mp'), may hold values from -0.21875 to 0.21875
- mlp_out: bfloat16 [2, 3072, 768], P(None, 'mp', 'dp'), may hold values from -0.109375 to 0.109375
- embodiment: int32 [96, 1], P('dp'), may hold values from 0 to 24; in each aligned block of 12 rows (0 to 11, 12 to 23, ...) no two rows name the same one
- levels: int32 [96, 2], P('dp'), may hold values from 0 to 19
- actions: bfloat16 [96, 2, 56], P('dp'), may hold values from -1 to 1
- noise: bfloat16 [96, 2, 56], P('dp'), may hold values from -5 to 5
- action_dims: int32 [25], replicated, may hold values from 7 to 14
- head_read: bfloat16 [32, 768, 256], P('dp'), may hold values from -0.21875 to 0.21875
- head_act: bfloat16 [32, 56, 256], P('dp'), may hold values from -0.75 to 0.75
- time_table: bfloat16 [32, 20, 256], P('dp'), may hold values from -5 to 5
- block_in: bfloat16 [32, 256, 256], P('dp'), may hold values from -0.375 to 0.375
- block_out: bfloat16 [32, 256, 256], P('dp'), may hold values from -0.375 to 0.375
- head_out: bfloat16 [32, 256, 56], P('dp'), may hold values from -0.375 to 0.375
Outputs:
- readout_grad: bfloat16 [96, 2, 768], P(('dp', 'mp'))
- grad_read: float32 [32, 768, 256], P('dp', 'mp')
- grad_act: float32 [32, 56, 256], P('dp')
- grad_time: float32 [32, 20, 256], P('dp')
- grad_block_in: float32 [32, 256, 256], P('dp')
- grad_block_out: float32 [32, 256, 256], P('dp')
- grad_head_out: float32 [32, 256, 56], P('dp')
The draws below stay inside these ranges and needn't reach their ends.
Inputs may be any that keep to these rules, and one draw needn't show every extreme that they name: Within each aligned block of 12 samples (those of one dp index) no embodiment appears twice; every embodiment appears in some block.
All inputs are finite; a program needn't handle non-finite values. No bound on the sum of `obs_mask` on one device may be relied on, other than what follows from the above.
Results may differ from the reference program's by a relative error of at most 0.024.
Values may be sent and summed in bfloat16 or wider, within the bound.
A program may use at most 64 MiB of HBM per device.

```python
import math
import jax
import jax.numpy as jnp
import numpy as np
from jax import lax

D = 768
HEADS = 12
HDIM = 64
FF = 3072
HID = 256
EMB = 25
LAYERS = 2
SEQ = 64
READ = 2
LEVELS = 20
ADIM_MAX = 14
SAMP_DEV = 12
SAMPLES = 96
TOKENS = 6144
EMB_SLOTS = 32
ACT = 56
N_DP = 8
N_MP = 4


def set_ends(result, key, smallest, high):
    dims = result.shape
    place = [jax.random.randint(jax.random.fold_in(key, axis), (), 0, dims[axis]) for axis in range(len(dims))]
    result = result.at[tuple(place)].set(smallest)
    longest = dims.index(max(dims))
    place[longest] = (place[longest] + 1) % dims[longest]
    return result.at[tuple(place)].set(high)


def steps_of(rng, shape, split, least, largest):
    gain, own = 1.0, jax.random.fold_in(rng, 6)
    for axis_at, parts in split:
        draws = jnp.exp(jax.random.uniform(jax.random.fold_in(own, axis_at), (parts,), jnp.float32, least / len(split), largest / len(split)))
        gain = gain * jnp.repeat(draws, shape[axis_at] // parts).reshape([-1 if axis == axis_at else 1 for axis in range(len(shape))])
    return gain


def routed_block(rng, own, number, rows, count, top, reach, lean):
    ranking = jax.random.permutation(rng, count)
    crowded, usual = load_shares(count, rows * top, reach, lean, True), load_shares(count, rows * top, reach, lean, False)
    places = jnp.arange(count)

    def named(lengths, rotation):
        used = int((lengths > 0).sum())
        fixed = max(1, used // 4)
        shifted = fixed + (places - fixed + rotation * (used - fixed)) % max(1, count - fixed)
        return jnp.zeros((count,), jnp.int32).at[ranking[jnp.where(places < fixed, places, shifted)]].set(jnp.asarray(lengths, jnp.int32))

    lengths = jnp.where(number % 4 == 0, named(crowded, number // 4), named(usual, number - number // 4 - 1))
    mixed = jax.random.permutation(jax.random.fold_in(own, 3), count)
    donor, taker = mixed[0:count // 2 * 2:2], mixed[1:count // 2 * 2:2]
    room = jnp.minimum(lengths[donor] - 1, reach - lengths[taker]) // 2
    room = jnp.where((donor == ranking[0]) | (taker == ranking[0]) | (lengths[taker] == 0), 0, jnp.maximum(room, 0))
    shifted = jax.random.randint(jax.random.fold_in(own, 4), (count // 2,), 0, 1 << 20) % (room + 1)
    lengths = lengths.at[donor].add(-shifted).at[taker].add(shifted)
    items = jnp.searchsorted(jnp.cumsum(lengths), jnp.arange(rows * top), side="right").astype(jnp.int32)
    grid = items.reshape(top, rows).T
    grid = grid[jax.random.permutation(jax.random.fold_in(own, 1), rows)]
    rotation = jax.random.randint(jax.random.fold_in(own, 2), (rows, 1), 0, top)
    return jnp.take_along_axis(grid, (jnp.arange(top)[None, :] + rotation) % top, axis=1)


def load_shares(count, total, reach, lean, full):
    weights = [(1 << 20) // math.isqrt(grade ** lean) + 1 for grade in range(1, count + 1)]
    largest = reach if full else min(reach, max(-(-total // count), total * weights[0] // sum(weights)))
    least = 1 if total - largest >= count - 1 else 0
    counts, surplus = [largest] + [least] * (count - 1), total - largest - least * (count - 1)
    while surplus > 0:
        movable = [i for i in range(1, count) if counts[i] < largest] or [i for i in range(1, count) if counts[i] < reach]
        whole, remaining = sum([weights[i] for i in movable]), surplus
        for i in movable:
            addition = min(reach - counts[i], max(1, remaining * weights[i] // whole), surplus)
            counts[i] = counts[i] + addition
            surplus = surplus - addition
    return np.array(counts)


def bell_draw(rng, dims, scale, reach, shards=(), kind=jnp.bfloat16):
    values = scale * jax.random.normal(rng, dims, jnp.float32)
    if shards:
        values = values * steps_of(rng, dims, shards, -0.22, 0.18)
    return jnp.clip(values, -reach, reach).astype(kind)


def setup_inputs(seed: int = 0) -> dict:
    arg_keys = jax.random.split(jax.random.key(seed), 19)
    tokens = bell_draw(arg_keys[0], (TOKENS, D), 1.0, 6.0, ((0, 32),))
    obs_mask = set_ends((jax.random.randint(arg_keys[1], (SAMPLES, SEQ), 0, 4) < 3).astype(jnp.int32), jax.random.fold_in(arg_keys[1], 1), 0, 1)
    norm_gains = jnp.clip(1.0 + 0.18 * jax.random.normal(arg_keys[2], (2 * LAYERS + 1, D), jnp.float32), 0.1, 1.9)
    attn_in = bell_draw(arg_keys[3], (LAYERS, 3, D, D), D ** -0.5, 0.21875, ((2, 8), (3, 4)))
    attn_out = bell_draw(arg_keys[4], (LAYERS, D, D), D ** -0.5, 0.21875, ((1, 4), (2, 8)))
    mlp_in = bell_draw(arg_keys[5], (LAYERS, D, FF), D ** -0.5, 0.21875, ((1, 8), (2, 4)))
    mlp_out = bell_draw(arg_keys[6], (LAYERS, FF, D), FF ** -0.5, 0.109375, ((1, 4), (2, 8)))
    embodiment_keys = jax.random.split(jax.random.fold_in(arg_keys[7], 1), SAMPLES // SAMP_DEV)
    embodiment_turns = jax.random.permutation(jax.random.fold_in(arg_keys[7], 3), SAMPLES // SAMP_DEV)
    embodiment = jax.vmap(lambda own, number: routed_block(jax.random.fold_in(arg_keys[7], 2), own, number, SAMP_DEV, EMB, 1, 1, 2))(embodiment_keys, embodiment_turns).reshape((SAMPLES, 1))
    levels = set_ends(jax.random.randint(arg_keys[8], (SAMPLES, READ), 0, LEVELS), jax.random.fold_in(arg_keys[8], 1), 0, LEVELS - 1).astype(jnp.int32)
    actions = jnp.clip(jax.random.uniform(arg_keys[9], (SAMPLES, READ, ACT), jnp.float32, -1.0, 1.0) * steps_of(arg_keys[9], (SAMPLES, READ, ACT), ((0, 8),), -0.4, 0.0), -1.0, 1.0).astype(jnp.bfloat16)
    noise = bell_draw(arg_keys[10], (SAMPLES, READ, ACT), 1.0, 5.0, ((0, 8),))
    action_dims = set_ends(jax.random.randint(arg_keys[11], (EMB,), 7, ADIM_MAX + 1), jax.random.fold_in(arg_keys[11], 1), 7, ADIM_MAX).astype(jnp.int32)
    head_read = bell_draw(arg_keys[12], (EMB_SLOTS, D, HID), D ** -0.5, 0.21875, ((0, 8),))
    head_act = bell_draw(arg_keys[13], (EMB_SLOTS, ACT, HID), ACT ** -0.5, 0.75, ((0, 8),))
    time_table = bell_draw(arg_keys[14], (EMB_SLOTS, LEVELS, HID), 1.0, 5.0, ((0, 8),))
    block_in = bell_draw(arg_keys[15], (EMB_SLOTS, HID, HID), HID ** -0.5, 0.375, ((0, 8),))
    block_out = bell_draw(arg_keys[16], (EMB_SLOTS, HID, HID), HID ** -0.5, 0.375, ((0, 8),))
    head_out = bell_draw(arg_keys[17], (EMB_SLOTS, HID, ACT), HID ** -0.5, 0.375, ((0, 8),))
    return {"tokens": tokens, "obs_mask": obs_mask, "norm_gains": norm_gains, "attn_in": attn_in, "attn_out": attn_out, "mlp_in": mlp_in, "mlp_out": mlp_out, "embodiment": embodiment, "levels": levels, "actions": actions, "noise": noise, "action_dims": action_dims, "head_read": head_read, "head_act": head_act, "time_table": time_table, "block_in": block_in, "block_out": block_out, "head_out": head_out}


norm_eps = 1e-05

def normalize(values, scale_gain):
    center = values - lax.optimization_barrier(jnp.mean(values, axis=-1, keepdims=True))
    spread = lax.optimization_barrier(jnp.mean(center * center, axis=-1, keepdims=True))
    return center * lax.rsqrt(spread + norm_eps) * scale_gain

def allowed_keys(observed):
    length = observed.shape[1]
    position = jnp.arange(length)
    visible = (observed == 1) & (position < length - READ)[None, :]
    itself = position[:, None] == position[None, :]
    return visible[:, None, :] | itself[None, :, :]

def attend(queries, key_rows, value_rows, allowed):
    scores = jnp.einsum('sqhd,skhd->shqk', queries.astype(jnp.float32), key_rows.astype(jnp.float32)) * HDIM ** (-0.5)
    weights = jnp.where(allowed[:, None, :, :], jnp.exp(scores), 0.0)
    shares = (weights / lax.optimization_barrier(jnp.sum(weights, axis=-1, keepdims=True))).astype(jnp.bfloat16)
    context = jnp.einsum('shqk,skhd->sqhd', shares.astype(jnp.float32), value_rows.astype(jnp.float32))
    return context.astype(jnp.bfloat16)

def split_sum(left_side, right_side, groups):
    part_width = left_side.shape[1] // groups
    summed = jnp.zeros((left_side.shape[0], right_side.shape[1]), jnp.float32)
    for part_index in range(groups):
        lower = part_index * part_width
        partial_value = jnp.dot(left_side[:, lower:lower + part_width], right_side[lower:lower + part_width], preferred_element_type=jnp.float32)
        summed = summed + lax.optimization_barrier(partial_value.astype(jnp.bfloat16)).astype(jnp.float32)
    return summed

def trunk_block(inputs, observed, norm_gains, attn_in, attn_out, mlp_in, mlp_out):
    residual = inputs.astype(jnp.float32)
    allowed = allowed_keys(observed)
    samples = observed.shape[0]
    for layer_index in range(LAYERS):
        normed = normalize(residual, norm_gains[2 * layer_index]).astype(jnp.bfloat16)
        projected = [jnp.dot(normed, attn_in[layer_index, member], preferred_element_type=jnp.float32).astype(jnp.bfloat16).reshape(samples, SEQ, HEADS, HDIM) for member in range(3)]
        context = attend(projected[0], projected[1], projected[2], allowed).reshape(-1, D)
        residual = residual + split_sum(context, attn_out[layer_index], N_MP)
        normed = normalize(residual, norm_gains[2 * layer_index + 1]).astype(jnp.bfloat16)
        hidden = jax.nn.gelu(jnp.dot(normed, mlp_in[layer_index], preferred_element_type=jnp.float32), approximate=True).astype(jnp.bfloat16)
        residual = residual + split_sum(hidden, mlp_out[layer_index], N_MP)
    ending = residual.reshape(samples, SEQ, D)[:, SEQ - READ:, :]
    return normalize(ending, norm_gains[2 * LAYERS]).astype(jnp.bfloat16)

def plan():
    steps_up = (jnp.arange(LEVELS, dtype=jnp.float32) + 1.0) / LEVELS
    anchor = math.cos(0.008 / 1.008 * math.pi / 2) ** 2
    return jnp.cos((steps_up + 0.008) / 1.008 * (math.pi / 2)) ** 2 / anchor

def noisy_pair(level_ids, clean, noise_draw, table):
    picked = (level_ids[..., None] == jnp.arange(LEVELS)).astype(jnp.float32)
    kept = lax.optimization_barrier(jnp.sum(picked * table, axis=-1))[..., None]
    mixed = jnp.sqrt(kept) * clean.astype(jnp.float32) + jnp.sqrt(1.0 - kept) * noise_draw.astype(jnp.float32)
    return mixed.astype(jnp.bfloat16)

def tail(first, target, weight_mask, inner_weight, outer_weight, final_weight):
    highest = lax.Precision.HIGHEST
    active = jax.nn.silu(first).astype(jnp.bfloat16)
    inner = jnp.dot(active, inner_weight, preferred_element_type=jnp.float32, precision=highest)
    second = jax.nn.silu(inner).astype(jnp.bfloat16)
    hidden = first + jnp.dot(second, outer_weight, preferred_element_type=jnp.float32, precision=highest)
    third = jax.nn.silu(hidden).astype(jnp.bfloat16)
    predicted = jnp.dot(third, final_weight, preferred_element_type=jnp.float32, precision=highest)
    differ = predicted - target
    return 0.5 * jnp.sum(weight_mask * differ * differ)

def reference(tokens, obs_mask, norm_gains, attn_in, attn_out, mlp_in, mlp_out, embodiment, levels, actions, noise, action_dims, head_read, head_act, time_table, block_in, block_out, head_out):

    def one_block(pieces):
        return trunk_block(pieces[0], pieces[1], norm_gains, attn_in, attn_out, mlp_in, mlp_out)
    blocks = lax.map(one_block, (tokens.reshape(N_DP, SAMP_DEV * SEQ, D), obs_mask.reshape(N_DP, SAMP_DEV, SEQ)))
    readouts = blocks.reshape(-1, D)
    table = plan()
    noisy = noisy_pair(levels, actions, noise, table).reshape(-1, ACT)
    target = noise.reshape(-1, ACT).astype(jnp.float32)
    level_rows = levels.reshape(-1)
    owner_rows = jnp.repeat(embodiment[:, 0], READ)
    one_hot = (level_rows[:, None] == jnp.arange(LEVELS)).astype(jnp.bfloat16)
    column = jnp.arange(ACT) % ADIM_MAX
    slot_count = head_read.shape[0]

    def per_head(carried, slot):
        read_weight = head_read[slot]
        live = (owner_rows == slot).astype(jnp.float32)
        dims_here = jnp.sum(jnp.where(jnp.arange(EMB) == slot, action_dims, 0))
        weight_mask = live[:, None] * (column[None, :] < dims_here).astype(jnp.float32)
        first = jnp.dot(readouts, read_weight, preferred_element_type=jnp.float32)
        first = first + jnp.dot(noisy, head_act[slot], preferred_element_type=jnp.float32)
        first = first + jnp.dot(one_hot, time_table[slot], preferred_element_type=jnp.float32)

        def head_loss(first_in, inner_weight, outer_weight, final_weight):
            return tail(first_in, target, weight_mask, inner_weight, outer_weight, final_weight)
        loss_value, pullback = jax.vjp(head_loss, first, block_in[slot].astype(jnp.float32), block_out[slot].astype(jnp.float32), head_out[slot].astype(jnp.float32))
        grad_first, grad_inner, grad_outer, grad_final = pullback(jnp.ones((), jnp.float32))
        grad_bf = grad_first.astype(jnp.bfloat16)
        grad_readin = jnp.dot(readouts.T, grad_bf, preferred_element_type=jnp.float32)
        grad_actin = jnp.dot(noisy.T, grad_bf, preferred_element_type=jnp.float32)
        grad_timein = jnp.dot(one_hot.T, grad_bf, preferred_element_type=jnp.float32)
        carried = carried + jnp.dot(grad_bf, read_weight.T, preferred_element_type=jnp.float32)
        return (carried, (grad_readin, grad_actin, grad_timein, grad_inner, grad_outer, grad_final))
    returned, grads = lax.scan(per_head, jnp.zeros(readouts.shape, jnp.float32), jnp.arange(slot_count))
    grad_readin, grad_actin, grad_timein, grad_inner, grad_outer, grad_final = grads
    return (returned.astype(jnp.bfloat16).reshape(SAMPLES, READ, D), grad_readin, grad_actin, grad_timein, grad_inner, grad_outer, grad_final)
```

```python
import functools
import math

import jax
import jax.numpy as jnp
from jax import lax
from jax.experimental import pallas as pl
from jax.experimental.pallas import tpu as pltpu
from jax.sharding import PartitionSpec as P

HDIM = 64
EMB = 25
READ = 2
LEVELS = 20
ADIM_MAX = 14

norm_eps = 1e-05
MESH_ID = pl.DeviceIdType.MESH


def normalize(values, scale_gain):
    center = values - jnp.mean(values, axis=-1, keepdims=True)
    spread = jnp.mean(center * center, axis=-1, keepdims=True)
    return center * lax.rsqrt(spread + norm_eps) * scale_gain


def plan():
    steps_up = (jnp.arange(LEVELS, dtype=jnp.float32) + 1.0) / LEVELS
    anchor = math.cos(0.008 / 1.008 * math.pi / 2) ** 2
    return jnp.cos((steps_up + 0.008) / 1.008 * (math.pi / 2)) ** 2 / anchor


def noisy_pair(level_ids, clean, noise_draw, table):
    picked = (level_ids[..., None] == jnp.arange(LEVELS)).astype(jnp.float32)
    kept = jnp.sum(picked * table, axis=-1)[..., None]
    mixed = jnp.sqrt(kept) * clean.astype(jnp.float32) + jnp.sqrt(1.0 - kept) * noise_draw.astype(
        jnp.float32
    )
    return mixed.astype(jnp.bfloat16)


def ring_place(index, size):
    if size % 2:
        return index
    odd = index % 2
    return (1 - odd) * (index // 2) + odd * (size - 1 - index // 2)


def ring_index(place, size):
    if size % 2:
        return place
    back = place // (size // 2)
    return (1 - back) * (2 * place) + back * (2 * (size - 1 - place) + 1)


def ring_parts(rows, tile=16):
    if rows % tile:
        return [(0, rows)]
    return [(start, tile) for start in range(0, rows, tile)]


def ring_step(parts, step, size):
    count = len(parts)
    if size % 2 == 0 and step == size // 2 - 1:
        near = (count + 1) // 2
        pairs = [(0, chunk) for chunk in range(near)], [(1, chunk) for chunk in range(near, count)]
        mixed = []
        for chunk in range(near):
            mixed += [side[chunk] for side in pairs if chunk < len(side)]
        return mixed
    return [(way, chunk) for chunk in range(count) for way in range(2)]


def exchange_kernel(n_dp, n_mp, kinds, *refs):
    count = len(kinds)
    ins, outs = refs[:count], refs[count : 2 * count]
    sems = refs[2 * count :]
    local_sem = sems[-1]
    my_dp, my_mp = lax.axis_index("dp"), lax.axis_index("mp")
    place = ring_place(my_dp, n_dp)

    talk_mp = any(kind in ("split", "cast") for kind in kinds)
    talk_dp = "swap" in kinds
    talk_ring = "ring" in kinds
    barrier = pltpu.get_barrier_semaphore()
    greeted = 0
    if talk_mp:
        for offset in range(1, n_mp):
            pl.semaphore_signal(
                barrier, inc=1, device_id={"mp": (my_mp + offset) % n_mp}, device_id_type=MESH_ID
            )
            greeted += 1
    if talk_dp:
        for offset in range(1, n_dp):
            pl.semaphore_signal(
                barrier, inc=1, device_id={"dp": (my_dp + offset) % n_dp}, device_id_type=MESH_ID
            )
            greeted += 1
    elif talk_ring:
        for way in (1, n_dp - 1):
            pl.semaphore_signal(
                barrier,
                inc=1,
                device_id={"dp": ring_index((place + way) % n_dp, n_dp)},
                device_id_type=MESH_ID,
            )
            greeted += 1
    pl.semaphore_wait(barrier, greeted)

    def ring_copies(item, step):
        source, landing = ins[item], outs[item]
        parts = ring_parts(source.shape[0])
        made = {}
        for way, chunk in ring_step(parts, step, n_dp):
            origin = ring_index((place + (n_dp - step if way == 0 else step)) % n_dp, n_dp)
            target = ring_index((place + (1 if way == 0 else n_dp - 1)) % n_dp, n_dp)
            rows = pl.ds(*parts[chunk])
            spot = landing.at[origin, rows]
            made[way, chunk] = pltpu.make_async_remote_copy(
                src_ref=source.at[rows] if step == 0 else spot,
                dst_ref=spot,
                send_sem=sems[2 * item].at[step, chunk, way],
                recv_sem=sems[2 * item + 1].at[step, chunk, way],
                device_id={"dp": target},
                device_id_type=MESH_ID,
            )
        return made

    rings = [item for item in range(count) if kinds[item] == "ring"]
    flights = {item: ring_copies(item, 0) for item in rings}
    for item in rings:
        for copy in flights[item].values():
            copy.start()
    direct = []
    keeps = []
    for item, kind in enumerate(kinds):
        source, landing = ins[item], outs[item]
        if kind == "ring":
            keeps.append(pltpu.make_async_copy(source, landing.at[my_dp], local_sem.at[item]))
            continue
        size, mine, axis = (n_dp, my_dp, "dp") if kind == "swap" else (n_mp, my_mp, "mp")
        for offset in range(1, size):
            peer = (mine + offset) % size
            copy = pltpu.make_async_remote_copy(
                src_ref=source if kind == "cast" else source.at[peer],
                dst_ref=landing.at[mine],
                send_sem=sems[2 * item].at[offset],
                recv_sem=sems[2 * item + 1].at[offset],
                device_id={axis: peer},
                device_id_type=MESH_ID,
            )
            copy.start()
            direct.append(copy)
        keeps.append(
            pltpu.make_async_copy(
                source if kind == "cast" else source.at[mine], landing.at[mine], local_sem.at[item]
            )
        )
    for keep in keeps:
        keep.start()
    sent = [copy for item in rings for copy in flights[item].values()]
    landed = []
    for step in range(1, n_dp // 2):
        for item in rings:
            following = ring_copies(item, step)
            for key, after in following.items():
                flights[item].pop(key).wait_recv()
                after.start()
            landed += flights[item].values()
            flights[item] = following
            sent += following.values()
    for item in rings:
        landed += flights[item].values()
    for copy in landed:
        copy.wait_recv()
    for copy in direct:
        copy.wait_recv()
    for copy in sent + direct:
        copy.wait_send()
    for keep in keeps:
        keep.wait()


def exchange(ident, *pairs):
    n_dp, n_mp = lax.axis_size("dp"), lax.axis_size("mp")
    kinds = tuple(kind for kind, _ in pairs)
    arrays = [array for _, array in pairs]
    shapes, scratch = [], []
    for kind, array in pairs:
        lead = {"ring": (n_dp,), "cast": (n_mp,), "split": (), "swap": ()}[kind]
        shapes.append(jax.ShapeDtypeStruct(lead + array.shape, array.dtype))
        if kind == "ring":
            slots = (n_dp // 2, len(ring_parts(array.shape[0])), 2)
        else:
            slots = (n_dp if kind == "swap" else n_mp,)
        scratch += [pltpu.SemaphoreType.DMA(slots), pltpu.SemaphoreType.DMA(slots)]
    scratch.append(pltpu.SemaphoreType.DMA((len(pairs),)))
    return pl.pallas_call(
        functools.partial(exchange_kernel, n_dp, n_mp, kinds),
        out_shape=shapes,
        in_specs=[pl.BlockSpec(memory_space=pltpu.VMEM)] * len(pairs),
        out_specs=[pl.BlockSpec(memory_space=pltpu.VMEM)] * len(pairs),
        scratch_shapes=scratch,
        compiler_params=pltpu.CompilerParams(collective_id=ident, has_side_effects=True),
        name="exchange%d" % ident,
    )(*arrays)


def attend(queries, key_rows, value_rows, allowed):
    scores = jnp.einsum(
        "sqhd,skhd->shqk", queries, key_rows, preferred_element_type=jnp.float32
    ) * HDIM ** (-0.5)
    weights = jnp.where(allowed[:, None, :, :], jnp.exp(scores), 0.0)
    shares = (weights / jnp.sum(weights, axis=-1, keepdims=True)).astype(jnp.bfloat16)
    context = jnp.einsum("shqk,skhd->sqhd", shares, value_rows, preferred_element_type=jnp.float32)
    return context.astype(jnp.bfloat16)


def dot32(left, right):
    return jnp.dot(left, right, preferred_element_type=jnp.float32)


def dot_turned(left, right):
    return lax.dot_general(
        left, right, (((1,), (1,)), ((), ())), preferred_element_type=jnp.float32
    )


def added(blocks):
    return jnp.sum(blocks.astype(jnp.float32), axis=0)


def tail(first, target, weight_mask, inner_weight, outer_weight, final_weight):
    highest = lax.Precision.HIGHEST
    active = jax.nn.silu(first).astype(jnp.bfloat16)
    inner = jnp.dot(active, inner_weight, preferred_element_type=jnp.float32, precision=highest)
    second = jax.nn.silu(inner).astype(jnp.bfloat16)
    hidden = first + jnp.dot(
        second, outer_weight, preferred_element_type=jnp.float32, precision=highest
    )
    third = jax.nn.silu(hidden).astype(jnp.bfloat16)
    predicted = jnp.dot(third, final_weight, preferred_element_type=jnp.float32, precision=highest)
    differ = predicted - target
    return 0.5 * jnp.sum(weight_mask * differ * differ)


def head_grads(first, inner_weight, outer_weight, final_weight, target, weight_mask):

    def head_loss(first_in, inner_in, outer_in, final_in):
        return tail(first_in, target, weight_mask, inner_in, outer_in, final_in)

    loss_value, pullback = jax.vjp(head_loss, first, inner_weight, outer_weight, final_weight)
    return pullback(jnp.ones((), jnp.float32))


CHUNK = 64


def remote(source, landing, send_sem, recv_sem, where):
    return pltpu.make_async_remote_copy(
        src_ref=source,
        dst_ref=landing,
        send_sem=send_sem,
        recv_sem=recv_sem,
        device_id=where,
        device_id_type=MESH_ID,
    )


def trunk_kernel(
    n_dp,
    n_mp,
    tokens,
    obs_mask,
    norm_gains,
    joined,
    raising,
    lowering,
    ends_out,
    full,
    cast_rows,
    residual,
    projected,
    context,
    hidden,
    partial_rows,
    near_part,
    far_part,
    own_part,
    paired,
    mask_all,
    ends_all,
    end_terms,
    out_weight,
    z_send,
    z_recv,
    y_send,
    y_recv,
    keep_sem,
    cast_send,
    cast_recv,
    sum_send,
    sum_recv,
    ends_send,
    ends_recv,
    term_send,
    term_recv,
    mask_send,
    mask_recv,
):
    layer_count = joined.shape[0]
    rows, model = residual.shape
    block = joined.shape[1]
    samples, length = obs_mask.shape
    width = model // n_mp
    wide = model // 3
    pad = wide - width
    heads = width // HDIM
    columns = n_dp // 2
    chunks = rows // CHUNK
    f32, bf16 = jnp.float32, jnp.bfloat16

    my_dp, my_mp = lax.axis_index("dp"), lax.axis_index("mp")
    my_z, my_y = my_dp // 2, my_dp % 2
    y_peer = {"dp": my_z * 2 + 1 - my_y}
    core = my_mp % 2
    sib = my_mp + 1 - 2 * core
    far = (my_mp + 2) % n_mp
    far_sib = (sib + 2) % n_mp
    sib_id, far_id = {"mp": sib}, {"mp": far}

    barrier = pltpu.get_barrier_semaphore()
    for offset in range(1, n_mp):
        pl.semaphore_signal(
            barrier, inc=1, device_id={"mp": (my_mp + offset) % n_mp}, device_id_type=MESH_ID
        )
    for offset in range(1, columns):
        pl.semaphore_signal(
            barrier,
            inc=1,
            device_id={"dp": ((my_z + offset) % columns) * 2 + my_y},
            device_id_type=MESH_ID,
        )
    pl.semaphore_signal(barrier, inc=1, device_id=y_peer, device_id_type=MESH_ID)

    def gain(index):
        return norm_gains[index : index + 1, :]

    def norm_chunk(index, chunk, gain_index):
        at = pl.ds(chunk * CHUNK, CHUNK)
        cast_rows[index, my_mp, at, :] = normalize(residual[at, :], gain(gain_index)).astype(bf16)

    for chunk in range(chunks):
        at = pl.ds(chunk * CHUNK, CHUNK)
        residual[at, :] = tokens[at, :].astype(f32)
        norm_chunk(0, chunk, 0)
    mask_all[my_mp] = obs_mask[...]
    pl.semaphore_wait(barrier, n_mp - 1 + columns)

    sources = [part.at[layer] for layer in range(layer_count) for part in (joined, raising, lowering)]

    def spot(unit, origin):
        return full.at[unit, pl.ds(pl.multiple_of(origin * block, block), block)]

    def z_copy(unit, offset):
        return remote(
            sources[unit],
            spot(unit, my_dp),
            z_send.at[unit, offset],
            z_recv.at[unit, offset],
            {"dp": ((my_z + offset) % columns) * 2 + my_y},
        )

    def z_landed(unit, offset):
        origin = ((my_z + columns - offset) % columns) * 2 + my_y
        return remote(
            sources[unit],
            spot(unit, origin),
            z_send.at[unit, offset],
            z_recv.at[unit, offset],
            {"dp": origin},
        )

    def y_copy(unit, offset):
        origin = ((my_z + columns - offset) % columns) * 2 + my_y
        return remote(
            sources[unit] if offset == 0 else spot(unit, origin),
            spot(unit, origin),
            y_send.at[unit, offset],
            y_recv.at[unit, offset],
            y_peer,
        )

    def y_landed(unit, offset):
        origin = ((my_z + columns - offset) % columns) * 2 + 1 - my_y
        return remote(
            sources[unit],
            spot(unit, origin),
            y_send.at[unit, offset],
            y_recv.at[unit, offset],
            y_peer,
        )

    def kept(unit):
        return pltpu.make_async_copy(sources[unit], spot(unit, my_dp), keep_sem.at[unit])

    def z_start(unit):
        for offset in range(1, columns):
            z_copy(unit, offset).start()
        kept(unit).start()

    def relay(unit, offset):
        z_landed(unit, offset).wait_recv()
        y_copy(unit, offset).start()

    def relay_all(unit):
        for offset in range(1, columns):
            relay(unit, offset)

    def complete(unit):
        for offset in range(columns):
            y_landed(unit, offset).wait_recv()
        kept(unit).wait()

    def cast_copy(index, way, chunk):
        at = pl.ds(chunk * CHUNK, CHUNK)
        whose = far if way == 2 else my_mp
        place = cast_rows.at[index, whose, at]
        return remote(
            place,
            place,
            cast_send.at[index, way, chunk],
            cast_recv.at[index, way, chunk],
            far_id if way == 1 else sib_id,
        )

    def cast_landed(index, way, chunk):
        at = pl.ds(chunk * CHUNK, CHUNK)
        place = cast_rows.at[index, (sib, far, far_sib)[way], at]
        return remote(
            place,
            place,
            cast_send.at[index, way, chunk],
            cast_recv.at[index, way, chunk],
            far_id if way == 1 else sib_id,
        )

    def cast_pass(index, chunk):
        cast_landed(index, 1, chunk).wait_recv()
        cast_copy(index, 2, chunk).start()

    def cast_near(index):
        for chunk in range(chunks):
            cast_landed(index, 0, chunk).wait_recv()

    def cast_far(index):
        for chunk in range(chunks):
            cast_landed(index, 2, chunk).wait_recv()

    def sum_near(index):
        return remote(
            partial_rows.at[far_sib],
            near_part.at[index],
            sum_send.at[index, 0, 0],
            sum_recv.at[index, 0, 0],
            sib_id,
        )

    def sum_own(index):
        return remote(
            partial_rows.at[sib],
            own_part.at[index],
            sum_send.at[index, 1, 0],
            sum_recv.at[index, 1, 0],
            sib_id,
        )

    def sum_far(index, chunk):
        at = pl.ds(chunk * CHUNK, CHUNK)
        return remote(
            paired.at[index, at],
            far_part.at[index, at],
            sum_send.at[index, 2, chunk],
            sum_recv.at[index, 2, chunk],
            far_id,
        )

    def sum_cross(index):
        sum_near(index).wait_recv()
        for chunk in range(chunks):
            at = pl.ds(chunk * CHUNK, CHUNK)
            paired[index, at, :] = (
                partial_rows[far, at, :].astype(f32) + near_part[index, at, :].astype(f32)
            ).astype(bf16)
            sum_far(index, chunk).start()

    def sum_finish(index, next_cast, gain_index):
        sum_own(index).wait_recv()
        for chunk in range(chunks):
            at = pl.ds(chunk * CHUNK, CHUNK)
            sum_far(index, chunk).wait_recv()
            residual[at, :] = (
                residual[at, :]
                + own_part[index, at, :].astype(f32)
                + far_part[index, at, :].astype(f32)
            )
            norm_chunk(next_cast, chunk, gain_index)
            cast_copy(next_cast, 1, chunk).start()
            cast_copy(next_cast, 0, chunk).start()

    def peers():
        return [(offset, {"mp": (my_mp + offset) % n_mp}) for offset in range(1, n_mp)]

    def ends_copy(offset, who):
        return remote(
            ends_all.at[my_mp], ends_all.at[my_mp], ends_send.at[offset], ends_recv.at[offset], who
        )

    def term_copy(index, offset, who):
        place = end_terms.at[index, my_mp]
        return remote(place, place, term_send.at[index, offset], term_recv.at[index, offset], who)

    def term_landed(index, offset):
        place = end_terms.at[index, (my_mp + n_mp - offset) % n_mp]
        return remote(
            place, place, term_send.at[index, offset], term_recv.at[index, offset], sib_id
        )

    def mask_copy(offset, who):
        return remote(
            obs_mask, mask_all.at[my_mp], mask_send.at[offset], mask_recv.at[offset], who
        )

    z_start(0)
    y_copy(0, 0).start()
    for offset, who in peers():
        mask_copy(offset, who).start()
    for chunk in range(chunks):
        cast_copy(0, 1, chunk).start()
        cast_copy(0, 0, chunk).start()
    z_start(1)
    for step in range(max(chunks, columns - 1)):
        if step < chunks:
            cast_pass(0, step)
        if step < columns - 1:
            relay(0, step + 1)
    y_copy(1, 0).start()
    z_start(2)

    lane = lax.broadcasted_iota(jnp.int32, (1, wide), 1)
    lane_masks = [
        jnp.where((lane >= head * HDIM) & (lane < (head + 1) * HDIM), 1.0, 0.0).astype(f32)
        for head in range(heads)
    ]

    def take_out_weight(unit):
        row = lax.broadcasted_iota(jnp.int32, (model, wide), 0)
        spot_lane = lax.broadcasted_iota(jnp.int32, (model, wide), 1)
        picks = (row % wide >= width) & (spot_lane == (row // wide) * pad + row % wide - width)
        choose = jnp.where(picks, 1.0, 0.0).astype(bf16)
        out_weight[...] = dot32(full[unit], choose).astype(bf16)

    def pair_rows(first, body):
        def step(index, carry):
            body(first + index)
            return carry

        lax.fori_loop(0, 2, step, 0)

    near_first = my_mp - core
    far_first = (near_first + 2) % n_mp

    def project(index, unit, owner):
        at = pl.ds(pl.multiple_of(owner * rows, rows), rows)
        projected[at, :] = dot32(cast_rows[index, owner], full[unit]).astype(bf16)

    def attention(tail_rows):
        asked = tail_rows if tail_rows else length
        row = lax.broadcasted_iota(jnp.int32, (heads * asked, length), 0) % asked
        col = lax.broadcasted_iota(jnp.int32, (heads * asked, length), 1)
        itself = jnp.where(row + (length - asked) == col, 1.0, 0.0)
        narrow = lax.broadcasted_iota(jnp.int32, (1, length), 1)

        def step(owner, carry):
            for sample in range(samples):
                start = owner * rows + sample * length
                at = pl.ds(pl.multiple_of(start, length), length)
                ask = pl.ds(pl.multiple_of(start + length - asked, 16), asked)
                query = projected[ask, :wide].astype(f32) * HDIM ** (-0.5)
                stacked = jnp.concatenate(
                    [(query * lanes).astype(bf16) for lanes in lane_masks], axis=0
                )
                scores = dot_turned(stacked, projected[at, wide : 2 * wide])
                seen = mask_all[owner, sample : sample + 1, :]
                seen = jnp.where((seen == 1) & (narrow < length - READ), 1.0, 0.0)
                weights = jnp.where(jnp.maximum(itself, seen) > 0.0, jnp.exp(scores), 0.0)
                shares = (weights / jnp.sum(weights, axis=-1, keepdims=True)).astype(bf16)
                mixed = dot32(shares, projected[at, 2 * wide :])
                total = mixed[:asked] * lane_masks[0]
                for head in range(1, heads):
                    total = total + mixed[head * asked : (head + 1) * asked] * lane_masks[head]
                put = pl.ds(
                    pl.multiple_of(owner * (samples * asked) + sample * asked, 16), asked
                )
                context[put, :] = total.astype(bf16)
            return carry

        lax.fori_loop(0, n_mp, step, 0)

    def combine(index, part_of, late):
        if index:
            sum_near(index - 1).wait_send()
            sum_own(index - 1).wait_send()
        partial_rows[far_sib] = part_of(far_sib).astype(bf16)
        sum_near(index).start()
        partial_rows[far] = part_of(far).astype(bf16)
        partial_rows[sib] = part_of(sib).astype(bf16)
        sum_own(index).start()
        sum_cross(index)
        residual[...] = residual[...] + part_of(my_mp)
        late()

    complete(0)
    cast_near(0)
    cast_far(0)
    for offset, who in peers():
        mask_copy(offset, who).wait_recv()
    take_out_weight(0)
    pair_rows(near_first, lambda owner: project(0, 0, owner))
    pair_rows(far_first, lambda owner: project(0, 0, owner))
    attention(0)

    def attended(owner):
        at = pl.ds(pl.multiple_of(owner * rows, rows), rows)
        return dot_turned(context[at, :], out_weight[...])

    def after_attention():
        relay_all(1)
        y_copy(2, 0).start()
        z_start(3)

    combine(0, attended, after_attention)
    sum_finish(0, 1, 1)
    for chunk in range(chunks):
        cast_pass(1, chunk)
    complete(1)

    def raise_rows(owner):
        hidden[owner] = jax.nn.gelu(dot32(cast_rows[1, owner], full[1]), approximate=True).astype(
            bf16
        )

    cast_near(1)
    pair_rows(near_first, raise_rows)
    relay_all(2)
    y_copy(3, 0).start()
    z_start(4)
    cast_far(1)
    pair_rows(far_first, raise_rows)
    complete(2)

    def lowered_rows(owner):
        return dot_turned(hidden[owner], full[2])

    def after_mlp():
        relay_all(3)
        y_copy(4, 0).start()
        z_start(5)

    combine(1, lowered_rows, after_mlp)
    sum_finish(1, 2, 2)
    ends_all[my_mp] = jnp.zeros(ends_all.shape[1:], f32)
    for sample in range(samples):
        last = (sample + 1) * length
        ends_all[my_mp, READ * sample : READ * (sample + 1), :] = residual[last - READ : last, :]
    for offset, who in peers():
        ends_copy(offset, who).start()
    for chunk in range(chunks):
        cast_pass(2, chunk)
    complete(3)
    take_out_weight(3)
    cast_near(2)
    pair_rows(near_first, lambda owner: project(2, 3, owner))
    relay_all(4)
    y_copy(5, 0).start()
    cast_far(2)
    pair_rows(far_first, lambda owner: project(2, 3, owner))
    attention(16)

    slots = ends_all.shape[1]
    row = lax.broadcasted_iota(jnp.int32, (n_mp * slots, n_mp * samples * 16), 0)
    col = lax.broadcasted_iota(jnp.int32, (n_mp * slots, n_mp * samples * 16), 1)
    inner = row % slots
    wanted = ((row // slots) * samples + inner // READ) * 16 + 16 - READ + inner % READ
    choose = jnp.where((wanted == col) & (inner < samples * READ), 1.0, 0.0).astype(bf16)
    ends_context = dot32(choose, context[: n_mp * samples * 16, :]).astype(bf16)

    def share(index, value):
        end_terms[index, my_mp] = value.astype(bf16)
        for offset, who in peers():
            term_copy(index, offset, who).start()

    def gathered_terms(index, ends):
        for offset in range(1, n_mp):
            term_landed(index, offset).wait_recv()
        for owner in range(n_mp):
            ends = ends + end_terms[index, owner].astype(f32)
        return ends

    share(0, dot_turned(ends_context, out_weight[...]))
    for offset, who in peers():
        remote(
            ends_all.at[my_mp],
            ends_all.at[(my_mp + n_mp - offset) % n_mp],
            ends_send.at[offset],
            ends_recv.at[offset],
            who,
        ).wait_recv()
    relay_all(5)
    ends = jnp.concatenate([ends_all[owner] for owner in range(n_mp)], axis=0)
    ends = gathered_terms(0, ends)
    normed = normalize(ends, gain(3)).astype(bf16)
    complete(4)
    raised = jax.nn.gelu(dot32(normed, full[4]), approximate=True).astype(bf16)
    complete(5)
    share(1, dot_turned(raised, full[5]))
    ends = gathered_terms(1, ends)
    ends_out[...] = normalize(ends, gain(4)).astype(bf16)

    for unit in range(len(sources)):
        for offset in range(columns):
            if offset:
                z_copy(unit, offset).wait_send()
            y_copy(unit, offset).wait_send()
    for index in range(3):
        for way in range(3):
            for chunk in range(chunks):
                cast_copy(index, way, chunk).wait_send()
    for index in range(2):
        if index == 1:
            sum_near(index).wait_send()
            sum_own(index).wait_send()
        for chunk in range(chunks):
            sum_far(index, chunk).wait_send()
    for offset, who in peers():
        mask_copy(offset, who).wait_send()
        ends_copy(offset, who).wait_send()
        for index in range(2):
            term_copy(index, offset, who).wait_send()


def trunk(tokens, obs_mask, norm_gains, joined, raising, lowering):
    n_dp, n_mp = lax.axis_size("dp"), lax.axis_size("mp")
    rows, model = tokens.shape
    samples = obs_mask.shape[0]
    wide = model // 3
    units = 3 * joined.shape[0]
    columns, chunks = n_dp // 2, rows // CHUNK
    slots = samples * READ + (-samples * READ) % 8
    bf16, f32 = jnp.bfloat16, jnp.float32
    dma = pltpu.SemaphoreType.DMA
    vmem = pltpu.VMEM
    return pl.pallas_call(
        functools.partial(trunk_kernel, n_dp, n_mp),
        out_shape=jax.ShapeDtypeStruct((n_mp * slots, model), bf16),
        in_specs=[pl.BlockSpec(memory_space=vmem)] * 6,
        out_specs=pl.BlockSpec(memory_space=vmem),
        scratch_shapes=[
            vmem((units, model, model), bf16),
            vmem((3, n_mp, rows, model), bf16),
            vmem((rows, model), f32),
            vmem((n_mp * rows, model), bf16),
            vmem((n_mp * rows, wide), bf16),
            vmem((n_mp, rows, model), bf16),
            vmem((n_mp, rows, model), bf16),
            vmem((2, rows, model), bf16),
            vmem((2, rows, model), bf16),
            vmem((2, rows, model), bf16),
            vmem((2, rows, model), bf16),
            vmem((n_mp,) + obs_mask.shape, jnp.int32),
            vmem((n_mp, slots, model), f32),
            vmem((2, n_mp, n_mp * slots, model), bf16),
            vmem((model, wide), bf16),
            dma((units, columns)),
            dma((units, columns)),
            dma((units, columns)),
            dma((units, columns)),
            dma((units,)),
            dma((3, 3, chunks)),
            dma((3, 3, chunks)),
            dma((2, 3, chunks)),
            dma((2, 3, chunks)),
            dma((n_mp,)),
            dma((n_mp,)),
            dma((2, n_mp)),
            dma((2, n_mp)),
            dma((n_mp,)),
            dma((n_mp,)),
        ],
        compiler_params=pltpu.CompilerParams(collective_id=50, has_side_effects=True),
        name="trunk",
    )(tokens, obs_mask, norm_gains, joined, raising, lowering)


def general_trunk(ident, tokens, obs_mask, norm_gains, attn_in, attn_out, mlp_in, mlp_out, small):
    model = tokens.shape[1]
    width = attn_in.shape[3]
    heads_local = width // HDIM
    samples_local, length = obs_mask.shape
    layer_count = attn_in.shape[0]
    n_mp = lax.axis_size("mp")
    samples_group = samples_local * n_mp
    joined = [
        jnp.concatenate(
            [attn_in[layer, 0], attn_in[layer, 1], attn_in[layer, 2], attn_out[layer].T], axis=1
        )
        for layer in range(layer_count)
    ]
    lowered = [mlp_out[layer].T for layer in range(layer_count)]


    residual = tokens.astype(jnp.float32)
    wide = None
    allowed = None
    mask_group = None
    got_small = None
    position = jnp.arange(length)
    for layer in range(layer_count):
        final = layer == layer_count - 1
        normed = normalize(residual, norm_gains[2 * layer]).astype(jnp.bfloat16)
        if layer == 0:
            sends = [("cast", normed), ("cast", obs_mask), ("swap", small), ("ring", joined[0])]
        else:
            sends = [("cast", normed)]
        if final:
            ends = residual.reshape(samples_local, length, model)[:, length - READ :, :]
            sends += [("cast", ends), ("ring", mlp_in[layer]), ("ring", lowered[layer])]
        got = list(exchange(next(ident), *sends))
        gathered = got.pop(0).reshape(-1, model)
        if layer == 0:
            mask_group = got.pop(0).reshape(samples_group, length)
            got_small = got.pop(0)
            wide = got.pop(0).reshape(model, -1)
            visible = (mask_group == 1) & (position < length - READ)[None, :]
            itself = position[:, None] == position[None, :]
            allowed = visible[:, None, :] | itself[None, :, :]
        if final:
            ends = got.pop(0).reshape(samples_group * READ, model)
            upper = got.pop(0).reshape(model, -1)
            lower = got.pop(0).reshape(model, -1)
            asking = gathered.reshape(samples_group, length, model)[:, length - READ :, :]
            queries = dot32(asking.reshape(-1, model), wide[:, :width]).astype(jnp.bfloat16)
            queries = queries.reshape(samples_group, READ, heads_local, HDIM)
            both = dot32(gathered, wide[:, width : 3 * width]).astype(jnp.bfloat16)
            keys_at = both[:, :width].reshape(samples_group, length, heads_local, HDIM)
            values_at = both[:, width:].reshape(samples_group, length, heads_local, HDIM)
            context = attend(queries, keys_at, values_at, allowed[:, length - READ :, :])
            partial_value = dot_turned(context.reshape(-1, width), wide[:, 3 * width :])
            (terms,) = exchange(next(ident), ("cast", partial_value.astype(jnp.bfloat16)))
            ends = ends + added(terms)
            normed = normalize(ends, norm_gains[2 * layer + 1]).astype(jnp.bfloat16)
            hidden = jax.nn.gelu(dot32(normed, upper), approximate=True).astype(jnp.bfloat16)
            partial_value = dot_turned(hidden, lower)
            (terms,) = exchange(next(ident), ("cast", partial_value.astype(jnp.bfloat16)))
            ends = ends + added(terms)
            break
        projected = dot32(gathered, wide[:, : 3 * width]).astype(jnp.bfloat16)
        split = [
            projected[:, part * width : (part + 1) * width].reshape(
                samples_group, length, heads_local, HDIM
            )
            for part in range(3)
        ]
        context = attend(split[0], split[1], split[2], allowed).reshape(-1, width)
        partial_value = dot_turned(context, wide[:, 3 * width :]).astype(jnp.bfloat16)
        terms, upper = exchange(
            next(ident),
            ("split", partial_value.reshape(n_mp, -1, model)),
            ("ring", mlp_in[layer]),
        )
        residual = residual + added(terms)
        normed = normalize(residual, norm_gains[2 * layer + 1]).astype(jnp.bfloat16)
        gathered, lower = exchange(next(ident), ("cast", normed), ("ring", lowered[layer]))
        raised = dot32(gathered.reshape(-1, model), upper.reshape(model, -1))
        hidden = jax.nn.gelu(raised, approximate=True).astype(jnp.bfloat16)
        partial_value = dot_turned(hidden, lower.reshape(model, -1)).astype(jnp.bfloat16)
        terms, wide = exchange(
            next(ident),
            ("split", partial_value.reshape(n_mp, -1, model)),
            ("ring", joined[layer + 1]),
        )
        wide = wide.reshape(model, -1)
        residual = residual + added(terms)

    return normalize(ends, norm_gains[2 * layer_count]).astype(jnp.bfloat16), got_small


def fused_trunk(ident, tokens, obs_mask, norm_gains, attn_in, attn_out, mlp_in, mlp_out, small):
    model = tokens.shape[1]
    width = attn_in.shape[3]
    pad = model // 3 - width
    samples_local = obs_mask.shape[0]
    n_mp = lax.axis_size("mp")
    pieces = []
    turned = jnp.swapaxes(attn_out, 1, 2)
    for part in range(3):
        pieces += [attn_in[:, part], turned[:, :, part * pad : (part + 1) * pad]]
    joined = jnp.concatenate(pieces, axis=2)
    ends = trunk(tokens, obs_mask, norm_gains, joined, mlp_in, jnp.swapaxes(mlp_out, 1, 2))
    ends = ends.reshape(n_mp, -1, model)[:, : samples_local * READ]
    return ends.reshape(-1, model), None


def fits_fused(tokens, obs_mask, attn_in, mlp_in):
    n_mp, n_dp = lax.axis_size("mp"), lax.axis_size("dp")
    model, width = tokens.shape[1], attn_in.shape[3]
    pad = model // 3 - width
    return (
        n_mp == 4
        and n_dp % 2 == 0
        and attn_in.shape[0] == 2
        and attn_in.shape[2] % 16 == 0
        and mlp_in.shape[2] == model
        and (model // 3) % 128 == 0
        and 3 * pad == width
        and tokens.shape[0] % CHUNK == 0
        and obs_mask.shape[1] == CHUNK
    )


def on_device(
    tokens,
    obs_mask,
    norm_gains,
    attn_in,
    attn_out,
    mlp_in,
    mlp_out,
    embodiment,
    levels,
    actions,
    noise,
    action_dims,
    head_read,
    head_act,
    time_table,
    block_in,
    block_out,
    head_out,
):
    model = tokens.shape[1]
    act = actions.shape[2]
    samples_local = obs_mask.shape[0]
    n_mp, n_dp = lax.axis_size("mp"), lax.axis_size("dp")
    my_model, my_owner = lax.axis_index("mp"), lax.axis_index("dp")
    samples_group = samples_local * n_mp
    ident = iter(range(100))

    heads_dev = head_read.shape[0]
    slot_count = heads_dev * n_dp
    owners = embodiment[:, 0]
    table = plan()
    onto = (jnp.arange(slot_count)[:, None] == owners[None, :]).astype(jnp.bfloat16)
    spread_rows = jnp.einsum("es,rq->ersq", onto, jnp.eye(READ, dtype=jnp.bfloat16)).reshape(
        slot_count * READ, samples_group * READ
    )
    small = jnp.concatenate(
        [
            noisy_pair(levels, actions, noise, table),
            noise,
            (levels + 1)[..., None].astype(jnp.bfloat16),
        ],
        axis=-1,
    ).reshape(samples_group * READ, 2 * act + 1)
    small = jnp.pad(small, ((0, 0), (0, -small.shape[1] % 128)))
    small = dot32(spread_rows, small).astype(jnp.bfloat16)
    small = small.reshape(n_dp, heads_dev * READ, small.shape[1])

    run = fused_trunk if fits_fused(tokens, obs_mask, attn_in, mlp_in) else general_trunk
    readouts, got_small = run(
        ident, tokens, obs_mask, norm_gains, attn_in, attn_out, mlp_in, mlp_out, small
    )
    send = dot32(spread_rows, readouts).astype(jnp.bfloat16)
    send = send.reshape(n_dp, heads_dev * READ, model)
    if got_small is None:
        got_features, got_small = exchange(next(ident), ("swap", send), ("swap", small))
    else:
        (got_features,) = exchange(next(ident), ("swap", send))

    def by_head(values):
        values = values.reshape(n_dp, heads_dev, READ, values.shape[-1])
        return jnp.moveaxis(values, 1, 0).reshape(heads_dev, n_dp * READ, values.shape[-1])

    head_features = by_head(got_features)
    head_small = by_head(got_small)
    head_noisy = head_small[..., :act]
    head_target = head_small[..., act : 2 * act].astype(jnp.float32)
    head_levels = head_small[..., 2 * act].astype(jnp.int32) - 1
    head_onehot = (head_levels[..., None] == jnp.arange(LEVELS)).astype(jnp.bfloat16)
    slot_ids = my_owner * heads_dev + jnp.arange(heads_dev)
    dims_here = jnp.sum(
        jnp.where(jnp.arange(EMB)[None, :] == slot_ids[:, None], action_dims[None, :], 0), axis=1
    )
    column = jnp.arange(act) % ADIM_MAX
    weight_mask = (head_levels >= 0).astype(jnp.float32)[..., None] * (
        column[None, None, :] < dims_here[:, None, None]
    ).astype(jnp.float32)
    others = jnp.einsum("hna,hac->hnc", head_noisy, head_act, preferred_element_type=jnp.float32)
    others = others + jnp.einsum(
        "hnl,hlc->hnc", head_onehot, time_table, preferred_element_type=jnp.float32
    )
    first = (
        jnp.einsum("hnd,hdc->hnc", head_features, head_read, preferred_element_type=jnp.float32)
        + others
    )
    grad_first, grad_inner, grad_outer, grad_final = jax.vmap(head_grads)(
        first,
        block_in.astype(jnp.float32),
        block_out.astype(jnp.float32),
        head_out.astype(jnp.float32),
        head_target,
        weight_mask,
    )
    grad_bf = grad_first.astype(jnp.bfloat16)
    backward = jnp.einsum(
        "hnc,hdc->hnd", grad_bf, head_read, preferred_element_type=jnp.float32
    ).astype(jnp.bfloat16)
    backward = jnp.moveaxis(backward.reshape(heads_dev, n_dp, READ, model), 0, 1)
    (arrived,) = exchange(
        next(ident), ("swap", backward.reshape(n_dp, heads_dev * READ, model))
    )
    mine = lax.dynamic_slice_in_dim(
        spread_rows, my_model * (samples_local * READ), samples_local * READ, 1
    )
    returned = lax.dot_general(
        mine,
        arrived.reshape(slot_count * READ, model),
        (((0,), (0,)), ((), ())),
        preferred_element_type=jnp.float32,
    ).astype(jnp.bfloat16)
    feature_width = model // n_mp
    own_features = lax.dynamic_slice_in_dim(
        head_features, my_model * feature_width, feature_width, 2
    )
    grad_readin = jnp.einsum(
        "hnd,hnc->hdc", own_features, grad_bf, preferred_element_type=jnp.float32
    )
    grad_actin = jnp.einsum("hna,hnc->hac", head_noisy, grad_bf, preferred_element_type=jnp.float32)
    grad_timein = jnp.einsum(
        "hnl,hnc->hlc", head_onehot, grad_bf, preferred_element_type=jnp.float32
    )
    return (
        returned.reshape(samples_local, READ, model),
        grad_readin,
        grad_actin,
        grad_timein,
        grad_inner,
        grad_outer,
        grad_final,
    )


def solution(mesh):
    placed = (
        P(("dp", "mp"), None),
        P(("dp", "mp"), None),
        P(),
        P(None, None, "dp", "mp"),
        P(None, "mp", "dp"),
        P(None, "dp", "mp"),
        P(None, "mp", "dp"),
        P("dp", None),
        P("dp", None),
        P("dp", None, None),
        P("dp", None, None),
        P(),
        P("dp", None, None),
        P("dp", None, None),
        P("dp", None, None),
        P("dp", None, None),
        P("dp", None, None),
        P("dp", None, None),
    )
    return jax.shard_map(
        on_device,
        mesh=mesh,
        in_specs=placed,
        out_specs=(
            P(("dp", "mp"), None, None),
            P("dp", "mp", None),
            P("dp", None, None),
            P("dp", None, None),
            P("dp", None, None),
            P("dp", None, None),
            P("dp", None, None),
        ),
        check_vma=False,
    )
```

```python
import functools
import math

import jax
import jax.numpy as jnp
from jax import lax
from jax.experimental import pallas as pl
from jax.experimental.pallas import tpu as pltpu
from jax.sharding import PartitionSpec as P

HDIM = 64
EMB = 25
READ = 2
LEVELS = 20
ADIM_MAX = 14

norm_eps = 1e-05
MESH_ID = pl.DeviceIdType.MESH


def normalize(values, scale_gain):
    center = values - jnp.mean(values, axis=-1, keepdims=True)
    spread = jnp.mean(center * center, axis=-1, keepdims=True)
    return center * lax.rsqrt(spread + norm_eps) * scale_gain


def plan():
    steps_up = (jnp.arange(LEVELS, dtype=jnp.float32) + 1.0) / LEVELS
    anchor = math.cos(0.008 / 1.008 * math.pi / 2) ** 2
    return jnp.cos((steps_up + 0.008) / 1.008 * (math.pi / 2)) ** 2 / anchor


def noisy_pair(level_ids, clean, noise_draw, table):
    picked = (level_ids[..., None] == jnp.arange(LEVELS)).astype(jnp.float32)
    kept = jnp.sum(picked * table, axis=-1)[..., None]
    mixed = jnp.sqrt(kept) * clean.astype(jnp.float32) + jnp.sqrt(1.0 - kept) * noise_draw.astype(
        jnp.float32
    )
    return mixed.astype(jnp.bfloat16)


def ring_place(index, size):
    if size % 2:
        return index
    odd = index % 2
    return (1 - odd) * (index // 2) + odd * (size - 1 - index // 2)


def ring_index(place, size):
    if size % 2:
        return place
    back = place // (size // 2)
    return (1 - back) * (2 * place) + back * (2 * (size - 1 - place) + 1)


def ring_parts(rows, tile=16):
    if rows % tile:
        return [(0, rows)]
    return [(start, tile) for start in range(0, rows, tile)]


def ring_step(parts, step, size):
    count = len(parts)
    if size % 2 == 0 and step == size // 2 - 1:
        near = (count + 1) // 2
        pairs = [(0, chunk) for chunk in range(near)], [(1, chunk) for chunk in range(near, count)]
        mixed = []
        for chunk in range(near):
            mixed += [side[chunk] for side in pairs if chunk < len(side)]
        return mixed
    return [(way, chunk) for chunk in range(count) for way in range(2)]


def exchange_kernel(n_dp, n_mp, kinds, *refs):
    count = len(kinds)
    ins, outs = refs[:count], refs[count : 2 * count]
    sems = refs[2 * count :]
    local_sem = sems[-1]
    my_dp, my_mp = lax.axis_index("dp"), lax.axis_index("mp")
    place = ring_place(my_dp, n_dp)

    talk_mp = any(kind in ("split", "cast") for kind in kinds)
    talk_dp = "swap" in kinds
    talk_ring = "ring" in kinds
    barrier = pltpu.get_barrier_semaphore()
    greeted = 0
    if talk_mp:
        for offset in range(1, n_mp):
            pl.semaphore_signal(
                barrier, inc=1, device_id={"mp": (my_mp + offset) % n_mp}, device_id_type=MESH_ID
            )
            greeted += 1
    if talk_dp:
        for offset in range(1, n_dp):
            pl.semaphore_signal(
                barrier, inc=1, device_id={"dp": (my_dp + offset) % n_dp}, device_id_type=MESH_ID
            )
            greeted += 1
    elif talk_ring:
        for way in (1, n_dp - 1):
            pl.semaphore_signal(
                barrier,
                inc=1,
                device_id={"dp": ring_index((place + way) % n_dp, n_dp)},
                device_id_type=MESH_ID,
            )
            greeted += 1
    pl.semaphore_wait(barrier, greeted)

    def ring_copies(item, step):
        source, landing = ins[item], outs[item]
        parts = ring_parts(source.shape[0])
        made = {}
        for way, chunk in ring_step(parts, step, n_dp):
            origin = ring_index((place + (n_dp - step if way == 0 else step)) % n_dp, n_dp)
            target = ring_index((place + (1 if way == 0 else n_dp - 1)) % n_dp, n_dp)
            rows = pl.ds(*parts[chunk])
            spot = landing.at[origin, rows]
            made[way, chunk] = pltpu.make_async_remote_copy(
                src_ref=source.at[rows] if step == 0 else spot,
                dst_ref=spot,
                send_sem=sems[2 * item].at[step, chunk, way],
                recv_sem=sems[2 * item + 1].at[step, chunk, way],
                device_id={"dp": target},
                device_id_type=MESH_ID,
            )
        return made

    rings = [item for item in range(count) if kinds[item] == "ring"]
    flights = {item: ring_copies(item, 0) for item in rings}
    for item in rings:
        for copy in flights[item].values():
            copy.start()
    direct = []
    keeps = []
    for item, kind in enumerate(kinds):
        source, landing = ins[item], outs[item]
        if kind == "ring":
            keeps.append(pltpu.make_async_copy(source, landing.at[my_dp], local_sem.at[item]))
            continue
        size, mine, axis = (n_dp, my_dp, "dp") if kind == "swap" else (n_mp, my_mp, "mp")
        for offset in range(1, size):
            peer = (mine + offset) % size
            copy = pltpu.make_async_remote_copy(
                src_ref=source if kind == "cast" else source.at[peer],
                dst_ref=landing.at[mine],
                send_sem=sems[2 * item].at[offset],
                recv_sem=sems[2 * item + 1].at[offset],
                device_id={axis: peer},
                device_id_type=MESH_ID,
            )
            copy.start()
            direct.append(copy)
        keeps.append(
            pltpu.make_async_copy(
                source if kind == "cast" else source.at[mine], landing.at[mine], local_sem.at[item]
            )
        )
    for keep in keeps:
        keep.start()
    sent = [copy for item in rings for copy in flights[item].values()]
    landed = []
    for step in range(1, n_dp // 2):
        for item in rings:
            following = ring_copies(item, step)
            for key, after in following.items():
                flights[item].pop(key).wait_recv()
                after.start()
            landed += flights[item].values()
            flights[item] = following
            sent += following.values()
    for item in rings:
        landed += flights[item].values()
    for copy in landed:
        copy.wait_recv()
    for copy in direct:
        copy.wait_recv()
    for copy in sent + direct:
        copy.wait_send()
    for keep in keeps:
        keep.wait()


def exchange(ident, *pairs):
    n_dp, n_mp = lax.axis_size("dp"), lax.axis_size("mp")
    kinds = tuple(kind for kind, _ in pairs)
    arrays = [array for _, array in pairs]
    shapes, scratch = [], []
    for kind, array in pairs:
        lead = {"ring": (n_dp,), "cast": (n_mp,), "split": (), "swap": ()}[kind]
        shapes.append(jax.ShapeDtypeStruct(lead + array.shape, array.dtype))
        if kind == "ring":
            slots = (n_dp // 2, len(ring_parts(array.shape[0])), 2)
        else:
            slots = (n_dp if kind == "swap" else n_mp,)
        scratch += [pltpu.SemaphoreType.DMA(slots), pltpu.SemaphoreType.DMA(slots)]
    scratch.append(pltpu.SemaphoreType.DMA((len(pairs),)))
    return pl.pallas_call(
        functools.partial(exchange_kernel, n_dp, n_mp, kinds),
        out_shape=shapes,
        in_specs=[pl.BlockSpec(memory_space=pltpu.VMEM)] * len(pairs),
        out_specs=[pl.BlockSpec(memory_space=pltpu.VMEM)] * len(pairs),
        scratch_shapes=scratch,
        compiler_params=pltpu.CompilerParams(collective_id=ident, has_side_effects=True),
        name="exchange%d" % ident,
    )(*arrays)


def attend(queries, key_rows, value_rows, allowed):
    scores = jnp.einsum(
        "sqhd,skhd->shqk", queries, key_rows, preferred_element_type=jnp.float32
    ) * HDIM ** (-0.5)
    weights = jnp.where(allowed[:, None, :, :], jnp.exp(scores), 0.0)
    shares = (weights / jnp.sum(weights, axis=-1, keepdims=True)).astype(jnp.bfloat16)
    context = jnp.einsum("shqk,skhd->sqhd", shares, value_rows, preferred_element_type=jnp.float32)
    return context.astype(jnp.bfloat16)


def dot32(left, right):
    return jnp.dot(left, right, preferred_element_type=jnp.float32)


def dot_turned(left, right):
    return lax.dot_general(
        left, right, (((1,), (1,)), ((), ())), preferred_element_type=jnp.float32
    )


def added(blocks):
    return jnp.sum(blocks.astype(jnp.float32), axis=0)


def tail(first, target, weight_mask, inner_weight, outer_weight, final_weight):
    highest = lax.Precision.HIGHEST
    active = jax.nn.silu(first).astype(jnp.bfloat16)
    inner = jnp.dot(active, inner_weight, preferred_element_type=jnp.float32, precision=highest)
    second = jax.nn.silu(inner).astype(jnp.bfloat16)
    hidden = first + jnp.dot(
        second, outer_weight, preferred_element_type=jnp.float32, precision=highest
    )
    third = jax.nn.silu(hidden).astype(jnp.bfloat16)
    predicted = jnp.dot(third, final_weight, preferred_element_type=jnp.float32, precision=highest)
    differ = predicted - target
    return 0.5 * jnp.sum(weight_mask * differ * differ)


def head_grads(first, inner_weight, outer_weight, final_weight, target, weight_mask):

    def head_loss(first_in, inner_in, outer_in, final_in):
        return tail(first_in, target, weight_mask, inner_in, outer_in, final_in)

    loss_value, pullback = jax.vjp(head_loss, first, inner_weight, outer_weight, final_weight)
    return pullback(jnp.ones((), jnp.float32))


CHUNK = 64
RING_STARTS = (0, 3, 4, 5, 6, 7)
RING_PARTS = 2
PUMPS = (1, 5, 5, 6, 7, 7, 8, 9, 9, 10)


def remote(source, landing, send_sem, recv_sem, where):
    return pltpu.make_async_remote_copy(
        src_ref=source,
        dst_ref=landing,
        send_sem=send_sem,
        recv_sem=recv_sem,
        device_id=where,
        device_id_type=MESH_ID,
    )


def trunk_kernel(
    n_dp,
    n_mp,
    tokens,
    obs_mask,
    norm_gains,
    attn_in,
    attn_out,
    raising,
    lowering,
    embodiment,
    levels,
    actions,
    noise,
    action_dims,
    read_hbm,
    act_hbm,
    time_hbm,
    inner_hbm,
    outer_hbm,
    final_hbm,
    back_out,
    read_out,
    act_out,
    time_out,
    inner_out,
    outer_out,
    final_out,
    full,
    cast_rows,
    residual,
    projected,
    context,
    hidden,
    partial_rows,
    near_part,
    far_part,
    own_part,
    paired,
    mask_all,
    ends_all,
    end_terms,
    out_weight,
    joined,
    returned,
    ring_send,
    ring_recv,
    keep_sem,
    cast_send,
    cast_recv,
    sum_send,
    sum_recv,
    ends_send,
    ends_recv,
    term_send,
    term_recv,
    mask_send,
    mask_recv,
    read_w,
    act_w,
    time_w,
    inner_w,
    outer_w,
    final_w,
    turned,
    small_out,
    small_in,
    rows_out,
    rows_in,
    back_rows,
    back_in,
    weight_sem,
    small_send,
    small_recv,
    rows_send,
    rows_recv,
    back_send,
    back_recv,
):
    layer_count = joined.shape[0]
    rows, model = residual.shape
    block = joined.shape[1]
    samples, length = obs_mask.shape
    width = model // n_mp
    wide = model // 3
    pad = wide - width
    heads = width // HDIM
    chunks = rows // CHUNK
    parts = ring_send.shape[2]
    f32, bf16 = jnp.float32, jnp.bfloat16

    my_dp, my_mp = lax.axis_index("dp"), lax.axis_index("mp")
    core = my_mp % 2
    sib = my_mp + 1 - 2 * core
    far = (my_mp + 2) % n_mp
    far_sib = (sib + 2) % n_mp
    sib_id, far_id = {"mp": sib}, {"mp": far}

    barrier = pltpu.get_barrier_semaphore()
    for offset in range(1, n_mp):
        pl.semaphore_signal(
            barrier, inc=1, device_id={"mp": (my_mp + offset) % n_mp}, device_id_type=MESH_ID
        )
    for offset in range(1, n_dp):
        pl.semaphore_signal(
            barrier, inc=1, device_id={"dp": (my_dp + offset) % n_dp}, device_id_type=MESH_ID
        )

    def gain(index):
        return norm_gains[index : index + 1, :]

    def norm_chunk(index, chunk, gain_index):
        at = pl.ds(chunk * CHUNK, CHUNK)
        cast_rows[index, my_mp, at, :] = normalize(residual[at, :], gain(gain_index)).astype(bf16)

    def flipped(left, right):
        return lax.dot_general(
            left, right, (((0,), (0,)), ((), ())), preferred_element_type=f32
        )

    piece_row = lax.broadcasted_iota(jnp.int32, (width, model), 0)
    piece_lane = lax.broadcasted_iota(jnp.int32, (width, model), 1)
    picks = piece_lane == (piece_row // pad) * wide + width + piece_row % pad
    placing = jnp.where(picks, 1.0, 0.0).astype(bf16)

    def join(layer):
        joined[layer] = flipped(attn_out[layer], placing).astype(bf16)
        for part in range(3):
            joined[layer, :, part * wide : part * wide + width] = attn_in[layer, part]

    join(0)
    for chunk in range(chunks):
        at = pl.ds(chunk * CHUNK, CHUNK)
        residual[at, :] = tokens[at, :].astype(f32)
        norm_chunk(0, chunk, 0)
    mask_all[my_mp] = obs_mask[...]
    pl.semaphore_wait(barrier, n_mp + n_dp - 2)

    sources = [part.at[layer] for layer in range(layer_count) for part in (joined, raising, lowering)]

    place = ring_place(my_dp, n_dp)
    half = n_dp // 2
    piece = block // parts

    def spot(unit, origin, part):
        return full.at[unit, pl.ds(pl.multiple_of(origin * block + part * piece, 16), piece)]

    def hop(unit, step, way, part):
        origin = ring_index((place + (n_dp - step if way == 0 else step)) % n_dp, n_dp)
        target = ring_index((place + (1 if way == 0 else n_dp - 1)) % n_dp, n_dp)
        here = spot(unit, origin, part)
        slot = step * 2 + way
        return remote(
            sources[unit].at[pl.ds(part * piece, piece)] if step == 0 else here,
            here,
            ring_send.at[unit, slot, part],
            ring_recv.at[unit, slot, part],
            {"dp": target},
        )

    def landed(unit, step, way, part):
        origin = ring_index(
            (place + (n_dp - step - 1 if way == 0 else step + 1)) % n_dp, n_dp
        )
        here = spot(unit, origin, part)
        slot = step * 2 + way
        return remote(
            here,
            here,
            ring_send.at[unit, slot, part],
            ring_recv.at[unit, slot, part],
            {"dp": ring_index((place + (1 if way == 0 else n_dp - 1)) % n_dp, n_dp)},
        )

    def legs(step):
        return [
            (way, part)
            for part in range(parts)
            for way in range(2)
            if step < half - 1 or (part < (parts + 1) // 2) == (way == 0)
        ]

    def kept(unit):
        return pltpu.make_async_copy(
            sources[unit],
            full.at[unit, pl.ds(pl.multiple_of(my_dp * block, block), block)],
            keep_sem.at[unit],
        )

    def tick(now):
        for unit in range(len(sources)):
            step = now - (RING_STARTS[unit])
            if step == 0:
                for way, part in legs(0):
                    hop(unit, 0, way, part).start()
                kept(unit).start()
            elif 0 < step <= half:
                after = legs(step) if step < half else []
                for way, part in legs(step - 1):
                    landed(unit, step - 1, way, part).wait_recv()
                    if (way, part) in after:
                        hop(unit, step, way, part).start()

    clock = [0]

    def pump(until):
        while clock[0] <= until:
            tick(clock[0])
            clock[0] += 1

    def complete(unit):
        pump(RING_STARTS[unit] + half)
        kept(unit).wait()

    def cast_copy(index, way, chunk):
        at = pl.ds(chunk * CHUNK, CHUNK)
        whose = far if way == 2 else my_mp
        place = cast_rows.at[index, whose, at]
        return remote(
            place,
            place,
            cast_send.at[index, way, chunk],
            cast_recv.at[index, way, chunk],
            far_id if way == 1 else sib_id,
        )

    def cast_landed(index, way, chunk):
        at = pl.ds(chunk * CHUNK, CHUNK)
        place = cast_rows.at[index, (sib, far, far_sib)[way], at]
        return remote(
            place,
            place,
            cast_send.at[index, way, chunk],
            cast_recv.at[index, way, chunk],
            far_id if way == 1 else sib_id,
        )

    def cast_pass(index, chunk):
        cast_landed(index, 1, chunk).wait_recv()
        cast_copy(index, 2, chunk).start()

    def cast_near(index):
        for chunk in range(chunks):
            cast_landed(index, 0, chunk).wait_recv()

    def cast_far(index):
        for chunk in range(chunks):
            cast_landed(index, 2, chunk).wait_recv()

    def sum_near(index):
        return remote(
            partial_rows.at[far_sib],
            near_part.at[index],
            sum_send.at[index, 0, 0],
            sum_recv.at[index, 0, 0],
            sib_id,
        )

    def sum_own(index):
        return remote(
            partial_rows.at[sib],
            own_part.at[index],
            sum_send.at[index, 1, 0],
            sum_recv.at[index, 1, 0],
            sib_id,
        )

    def sum_far(index, chunk):
        at = pl.ds(chunk * CHUNK, CHUNK)
        return remote(
            paired.at[index, at],
            far_part.at[index, at],
            sum_send.at[index, 2, chunk],
            sum_recv.at[index, 2, chunk],
            far_id,
        )

    def sum_cross(index):
        sum_near(index).wait_recv()
        for chunk in range(chunks):
            at = pl.ds(chunk * CHUNK, CHUNK)
            paired[index, at, :] = (
                partial_rows[far, at, :].astype(f32) + near_part[index, at, :].astype(f32)
            ).astype(bf16)
            sum_far(index, chunk).start()

    def sum_finish(index, next_cast, gain_index):
        sum_own(index).wait_recv()
        for chunk in range(chunks):
            at = pl.ds(chunk * CHUNK, CHUNK)
            sum_far(index, chunk).wait_recv()
            residual[at, :] = (
                residual[at, :]
                + own_part[index, at, :].astype(f32)
                + far_part[index, at, :].astype(f32)
            )
            norm_chunk(next_cast, chunk, gain_index)
            cast_copy(next_cast, 1, chunk).start()
            cast_copy(next_cast, 0, chunk).start()

    def peers():
        return [(offset, {"mp": (my_mp + offset) % n_mp}) for offset in range(1, n_mp)]

    def ends_copy(offset, who):
        return remote(
            ends_all.at[my_mp], ends_all.at[my_mp], ends_send.at[offset], ends_recv.at[offset], who
        )

    def term_copy(index, offset, who):
        place = end_terms.at[index, my_mp]
        return remote(place, place, term_send.at[index, offset], term_recv.at[index, offset], who)

    def term_landed(index, offset):
        place = end_terms.at[index, (my_mp + n_mp - offset) % n_mp]
        return remote(
            place, place, term_send.at[index, offset], term_recv.at[index, offset], sib_id
        )

    def mask_copy(offset, who):
        return remote(
            obs_mask, mask_all.at[my_mp], mask_send.at[offset], mask_recv.at[offset], who
        )

    def swap_copy(source, landing, send_sem, recv_sem, offset):
        peer = (my_dp + offset) % n_dp
        return remote(
            source.at[peer],
            landing.at[my_dp],
            send_sem.at[offset],
            recv_sem.at[offset],
            {"dp": peer},
        )

    def swap_landed(source, landing, send_sem, recv_sem, offset):
        peer = (my_dp + n_dp - offset) % n_dp
        return remote(
            source.at[peer],
            landing.at[peer],
            send_sem.at[offset],
            recv_sem.at[offset],
            {"dp": peer},
        )

    def swap_start(*swap):
        for offset in range(1, n_dp):
            swap_copy(*swap, offset).start()
        swap[1][my_dp] = swap[0][my_dp]

    def swap_wait(*swap):
        for offset in range(1, n_dp):
            swap_landed(*swap, offset).wait_recv()

    small_swap = (small_out, small_in, small_send, small_recv)
    rows_swap = (rows_out, rows_in, rows_send, rows_recv)
    back_swap = (back_rows, back_in, back_send, back_recv)
    head_count, slot_rows = read_hbm.shape[0], rows_in.shape[1]
    all_rows = n_dp * slot_rows
    weight_copies = [
        pltpu.make_async_copy(source, landing, weight_sem.at[index])
        for index, (source, landing) in enumerate(
            (
                (read_hbm, read_w),
                (act_hbm, act_w),
                (time_hbm, time_w),
                (inner_hbm, inner_w),
                (outer_hbm, outer_w),
                (final_hbm, final_w),
            )
        )
    ]

    pump(0)
    for offset, who in peers():
        mask_copy(offset, who).start()
    for chunk in range(chunks):
        cast_copy(0, 1, chunk).start()
        cast_copy(0, 0, chunk).start()
    for copy in weight_copies:
        copy.start()
    join(1)
    group = levels.shape[1]
    act = actions.shape[2]
    tile = 128
    slots = ends_all.shape[1]
    end_rows = n_mp * slots
    slot_of = lax.broadcasted_iota(jnp.int32, (all_rows, group), 0)
    sample_at = lax.broadcasted_iota(jnp.int32, (group, end_rows), 0)
    end_of = lax.broadcasted_iota(jnp.int32, (group, end_rows), 1)
    end_sample = (end_of // slots) * samples + end_of % slots // READ
    end_here = (end_sample == sample_at) & (end_of % slots < samples * READ)
    square = lax.broadcasted_iota(jnp.int32, (group, group), 0)
    square = square == lax.broadcasted_iota(jnp.int32, (group, group), 1)
    level_lane = lax.broadcasted_iota(jnp.int32, (group, tile), 1)
    table_lane = lax.broadcasted_iota(jnp.int32, (1, tile), 1)
    table = jnp.zeros((1, tile), f32)
    for level, value in enumerate(plan_values()):
        table = jnp.where(table_lane == level, value, table)
    spread = jnp.zeros((all_rows, end_rows), f32)
    scattered = [jnp.zeros((all_rows, act), f32)] * 2 + [jnp.zeros((all_rows, tile), f32)]
    clean_all, noise_all = actions[...].astype(f32), noise[...].astype(f32)
    for read in range(READ):
        route = (embodiment[...] == slot_of // READ) & (slot_of % READ == read)
        route = jnp.where(route, 1.0, 0.0).astype(bf16)
        ends_here = jnp.where(end_here & (end_of % READ == read), 1.0, 0.0).astype(bf16)
        spread = spread + dot32(route, ends_here)
        level = jnp.sum(
            jnp.where(square, levels[read : read + 1, :], 0), axis=1, keepdims=True
        )
        onehot = jnp.where(level_lane == level, 1.0, 0.0)
        kept_share = jnp.sum(onehot * table, axis=1, keepdims=True)
        clean, drawn = clean_all[:, read, :], noise_all[:, read, :]
        mixed = jnp.sqrt(kept_share) * clean + jnp.sqrt(1.0 - kept_share) * drawn
        for index, values in enumerate((mixed, drawn, onehot)):
            scattered[index] = scattered[index] + dot32(route, values.astype(bf16))
    spread = spread.astype(bf16)
    small_out[...] = jnp.zeros(small_out.shape, bf16)
    for peer in range(n_dp):
        at = slice(peer * slot_rows, (peer + 1) * slot_rows)
        for index, values in enumerate(scattered):
            columns = slice(index * tile, index * tile + values.shape[1])
            small_out[peer, :, columns] = values[at].astype(bf16)
    swap_start(*small_swap)
    for chunk in range(chunks):
        cast_pass(0, chunk)
        pump(PUMPS[0] + chunk)

    lane = lax.broadcasted_iota(jnp.int32, (1, wide), 1)
    lane_masks = [
        jnp.where((lane >= head * HDIM) & (lane < (head + 1) * HDIM), 1.0, 0.0).astype(f32)
        for head in range(heads)
    ]

    def take_out_weight(unit):
        row = lax.broadcasted_iota(jnp.int32, (model, wide), 0)
        spot_lane = lax.broadcasted_iota(jnp.int32, (model, wide), 1)
        picks = (row % wide >= width) & (spot_lane == (row // wide) * pad + row % wide - width)
        choose = jnp.where(picks, 1.0, 0.0).astype(bf16)
        out_weight[...] = dot32(full[unit], choose).astype(bf16)

    def pair_rows(first, body):
        def step(index, carry):
            body(first + index)
            return carry

        lax.fori_loop(0, 2, step, 0)

    near_first = my_mp - core
    far_first = (near_first + 2) % n_mp

    def project(index, unit, owner):
        at = pl.ds(pl.multiple_of(owner * rows, rows), rows)
        projected[at, :] = dot32(cast_rows[index, owner], full[unit]).astype(bf16)

    def attention(tail_rows):
        asked = tail_rows if tail_rows else length
        row = lax.broadcasted_iota(jnp.int32, (heads * asked, length), 0) % asked
        col = lax.broadcasted_iota(jnp.int32, (heads * asked, length), 1)
        itself = jnp.where(row + (length - asked) == col, 1.0, 0.0)
        narrow = lax.broadcasted_iota(jnp.int32, (1, length), 1)

        def step(owner, carry):
            for sample in range(samples):
                start = owner * rows + sample * length
                at = pl.ds(pl.multiple_of(start, length), length)
                ask = pl.ds(pl.multiple_of(start + length - asked, 16), asked)
                query = projected[ask, :wide].astype(f32) * HDIM ** (-0.5)
                stacked = jnp.concatenate(
                    [(query * lanes).astype(bf16) for lanes in lane_masks], axis=0
                )
                scores = dot_turned(stacked, projected[at, wide : 2 * wide])
                seen = mask_all[owner, sample : sample + 1, :]
                seen = jnp.where((seen == 1) & (narrow < length - READ), 1.0, 0.0)
                weights = jnp.where(jnp.maximum(itself, seen) > 0.0, jnp.exp(scores), 0.0)
                shares = (weights / jnp.sum(weights, axis=-1, keepdims=True)).astype(bf16)
                mixed = dot32(shares, projected[at, 2 * wide :])
                total = mixed[:asked] * lane_masks[0]
                for head in range(1, heads):
                    total = total + mixed[head * asked : (head + 1) * asked] * lane_masks[head]
                put = pl.ds(
                    pl.multiple_of(owner * (samples * asked) + sample * asked, 16), asked
                )
                context[put, :] = total.astype(bf16)
            return carry

        lax.fori_loop(0, n_mp, step, 0)

    def combine(index, part_of, late):
        if index:
            sum_near(index - 1).wait_send()
            sum_own(index - 1).wait_send()
        partial_rows[far_sib] = part_of(far_sib).astype(bf16)
        sum_near(index).start()
        partial_rows[far] = part_of(far).astype(bf16)
        partial_rows[sib] = part_of(sib).astype(bf16)
        sum_own(index).start()
        sum_cross(index)
        residual[...] = residual[...] + part_of(my_mp)
        late()

    complete(0)
    cast_near(0)
    cast_far(0)
    for offset, who in peers():
        mask_copy(offset, who).wait_recv()
    take_out_weight(0)
    pair_rows(near_first, lambda owner: project(0, 0, owner))
    pair_rows(far_first, lambda owner: project(0, 0, owner))
    pump(PUMPS[1])
    attention(0)
    pump(PUMPS[2])

    def attended(owner):
        at = pl.ds(pl.multiple_of(owner * rows, rows), rows)
        return dot_turned(context[at, :], out_weight[...])

    def after_attention():
        pump(PUMPS[3])

    combine(0, attended, after_attention)
    sum_finish(0, 1, 1)
    for chunk in range(chunks):
        cast_pass(1, chunk)
    pump(PUMPS[4])
    complete(1)

    def raise_rows(owner):
        hidden[owner] = jax.nn.gelu(dot32(cast_rows[1, owner], full[1]), approximate=True).astype(
            bf16
        )

    cast_near(1)
    pair_rows(near_first, raise_rows)
    pump(PUMPS[5])
    cast_far(1)
    pair_rows(far_first, raise_rows)
    complete(2)

    def lowered_rows(owner):
        return dot_turned(hidden[owner], full[2])

    def after_mlp():
        pump(PUMPS[6])

    combine(1, lowered_rows, after_mlp)
    sum_finish(1, 2, 2)
    ends_all[my_mp] = jnp.zeros(ends_all.shape[1:], f32)
    for sample in range(samples):
        last = (sample + 1) * length
        ends_all[my_mp, READ * sample : READ * (sample + 1), :] = residual[last - READ : last, :]
    for offset, who in peers():
        ends_copy(offset, who).start()
    for chunk in range(chunks):
        cast_pass(2, chunk)
    pump(PUMPS[7])
    complete(3)
    take_out_weight(3)
    cast_near(2)
    pair_rows(near_first, lambda owner: project(2, 3, owner))
    pump(PUMPS[8])
    cast_far(2)
    pair_rows(far_first, lambda owner: project(2, 3, owner))
    attention(16)
    pump(PUMPS[9])

    row = lax.broadcasted_iota(jnp.int32, (n_mp * slots, n_mp * samples * 16), 0)
    col = lax.broadcasted_iota(jnp.int32, (n_mp * slots, n_mp * samples * 16), 1)
    inner = row % slots
    wanted = ((row // slots) * samples + inner // READ) * 16 + 16 - READ + inner % READ
    choose = jnp.where((wanted == col) & (inner < samples * READ), 1.0, 0.0).astype(bf16)
    ends_context = dot32(choose, context[: n_mp * samples * 16, :]).astype(bf16)

    def share(index, value):
        end_terms[index, my_mp] = value.astype(bf16)
        for offset, who in peers():
            term_copy(index, offset, who).start()

    def gathered_terms(index, ends):
        for offset in range(1, n_mp):
            term_landed(index, offset).wait_recv()
        for owner in range(n_mp):
            ends = ends + end_terms[index, owner].astype(f32)
        return ends

    share(0, dot_turned(ends_context, out_weight[...]))
    for offset, who in peers():
        remote(
            ends_all.at[my_mp],
            ends_all.at[(my_mp + n_mp - offset) % n_mp],
            ends_send.at[offset],
            ends_recv.at[offset],
            who,
        ).wait_recv()
    ends = jnp.concatenate([ends_all[owner] for owner in range(n_mp)], axis=0)
    ends = gathered_terms(0, ends)
    normed = normalize(ends, gain(3)).astype(bf16)
    complete(4)
    raised = jax.nn.gelu(dot32(normed, full[4]), approximate=True).astype(bf16)
    complete(5)
    share(1, dot_turned(raised, full[5]))
    ends = gathered_terms(1, ends)
    readouts = normalize(ends, gain(4)).astype(bf16)

    scattered = dot32(spread, readouts)
    for peer in range(n_dp):
        rows_out[peer] = scattered[peer * slot_rows : (peer + 1) * slot_rows].astype(bf16)
    swap_start(*rows_swap)
    for copy in weight_copies:
        copy.wait()
    swap_wait(*small_swap)
    facts = jnp.concatenate([small_in[peer].astype(f32) for peer in range(n_dp)], axis=0)
    noisy = facts[:, :tile].astype(bf16)
    target = facts[:, tile : tile + act]
    onehot = facts[:, 2 * tile :].astype(bf16)
    row_of = lax.broadcasted_iota(jnp.int32, (all_rows, act), 0) % slot_rows // READ
    live = jnp.sum(facts[:, 2 * tile :], axis=1, keepdims=True)
    column = lax.broadcasted_iota(jnp.int32, (1, act), 1) % ADIM_MAX
    times = time_w[...].astype(f32)
    firsts = [
        dot32(noisy[:, :act], act_w[head]) + dot32(onehot[:, :LEVELS], times[:, head, :].astype(bf16))
        for head in range(head_count)
    ]
    swap_wait(*rows_swap)
    features = jnp.concatenate([rows_in[peer].astype(f32) for peer in range(n_dp)], axis=0)
    features = features.astype(bf16)

    def slope(value):
        gate = jax.nn.sigmoid(value)
        return gate * (1.0 + value * (1.0 - gate))

    kept_back = []
    backward = jnp.zeros((all_rows, model), f32)
    for head in range(head_count):
        first = firsts[head] + dot32(features, read_w[head])
        active = jax.nn.silu(first).astype(bf16)
        inner = dot32(active, inner_w[head])
        second = jax.nn.silu(inner).astype(bf16)
        above = first + dot32(second, outer_w[head])
        third = jax.nn.silu(above).astype(bf16)
        predicted = dot_turned(third, final_w[head])
        slot = my_dp * head_count + head
        dims = jnp.where(slot < EMB, action_dims[jnp.minimum(slot, EMB - 1)], 0)
        mask = jnp.where((row_of == head) & (column < dims), live, 0.0)
        differ = (mask * (predicted - target)).astype(bf16)
        above_grad = dot32(differ, final_w[head]).astype(bf16).astype(f32) * slope(above)
        above_bf = above_grad.astype(bf16)
        inner_grad = dot_turned(above_bf, outer_w[head]).astype(bf16).astype(f32) * slope(inner)
        inner_bf = inner_grad.astype(bf16)
        first_grad = above_grad + dot_turned(inner_bf, inner_w[head]).astype(bf16).astype(
            f32
        ) * slope(first)
        first_bf = first_grad.astype(bf16)
        backward = backward + dot_turned(first_bf, read_w[head])
        kept_back.append((active, second, third, differ, above_bf, inner_bf, first_bf))
    for peer in range(n_dp):
        back_rows[peer] = backward[peer * slot_rows : (peer + 1) * slot_rows].astype(bf16)
    swap_start(*back_swap)

    turned[...] = jnp.transpose(features.astype(f32)).astype(bf16)
    own_features = turned[pl.ds(pl.multiple_of(my_mp * width, 16), width), :]
    for head, kept_now in enumerate(kept_back):
        active, second, third, differ, above_bf, inner_bf, first_bf = kept_now
        read_out[head] = dot32(own_features, first_bf)
        act_out[head] = flipped(noisy, first_bf)[:act]
        time_out[:, head, :] = flipped(onehot, first_bf)[:LEVELS]
        inner_out[head] = flipped(active, inner_bf)
        outer_out[head] = flipped(second, above_bf)
        final_out[head] = flipped(differ, third)
    swap_wait(*back_swap)
    arrived = jnp.concatenate([back_in[peer].astype(f32) for peer in range(n_dp)], axis=0)
    arrived = flipped(spread, arrived.astype(bf16))
    for owner in range(n_mp):
        returned[owner] = arrived[owner * slots : (owner + 1) * slots]
    mine = returned[my_mp]
    for sample in range(samples):
        back_out[sample] = mine[READ * sample : READ * (sample + 1)].astype(bf16)

    for unit in range(len(sources)):
        for step in range(half):
            for way, part in legs(step):
                hop(unit, step, way, part).wait_send()
    for offset in range(1, n_dp):
        swap_copy(*small_swap, offset).wait_send()
        swap_copy(*rows_swap, offset).wait_send()
        swap_copy(*back_swap, offset).wait_send()
    for index in range(3):
        for way in range(3):
            for chunk in range(chunks):
                cast_copy(index, way, chunk).wait_send()
    for index in range(2):
        if index == 1:
            sum_near(index).wait_send()
            sum_own(index).wait_send()
        for chunk in range(chunks):
            sum_far(index, chunk).wait_send()
    for offset, who in peers():
        mask_copy(offset, who).wait_send()
        ends_copy(offset, who).wait_send()
        for index in range(2):
            term_copy(index, offset, who).wait_send()


def plan_values():
    anchor = math.cos(0.008 / 1.008 * math.pi / 2) ** 2
    steps = [(level + 1.0) / LEVELS for level in range(LEVELS)]
    return [math.cos((up + 0.008) / 1.008 * math.pi / 2) ** 2 / anchor for up in steps]


def trunk(
    tokens,
    obs_mask,
    norm_gains,
    attn_in,
    attn_out,
    raising,
    lowering,
    embodiment,
    levels,
    actions,
    noise,
    action_dims,
    *head_weights,
):
    n_dp, n_mp = lax.axis_size("dp"), lax.axis_size("mp")
    rows, model = tokens.shape
    samples = obs_mask.shape[0]
    wide = model // 3
    units = 3 * raising.shape[0]
    chunks = rows // CHUNK
    parts = RING_PARTS if raising.shape[1] % (16 * RING_PARTS) == 0 else 1
    slots = samples * READ + (-samples * READ) % 8
    heads = head_weights[0].shape[0]
    bf16, f32 = jnp.bfloat16, jnp.float32
    dma = pltpu.SemaphoreType.DMA
    vmem = pltpu.VMEM
    inner_spec = pl.BlockSpec(memory_space=vmem)
    outer_spec = pl.BlockSpec(memory_space=pl.ANY)
    grads = []
    for index, weight in enumerate(head_weights):
        shape = weight.shape if index else (heads, model // n_mp, weight.shape[2])
        grads.append(jax.ShapeDtypeStruct(shape, f32))
    per_owner = heads * READ
    return pl.pallas_call(
        functools.partial(trunk_kernel, n_dp, n_mp),
        out_shape=[jax.ShapeDtypeStruct((samples, READ, model), bf16)] + grads,
        in_specs=[inner_spec] * 11
        + [pl.BlockSpec(memory_space=pltpu.SMEM)]
        + [outer_spec] * len(head_weights),
        out_specs=[inner_spec] * (1 + len(grads)),
        scratch_shapes=[
            vmem((units, model, model), bf16),
            vmem((3, n_mp, rows, model), bf16),
            vmem((rows, model), f32),
            vmem((n_mp * rows, model), bf16),
            vmem((n_mp * rows, wide), bf16),
            vmem((n_mp, rows, model), bf16),
            vmem((n_mp, rows, model), bf16),
            vmem((2, rows, model), bf16),
            vmem((2, rows, model), bf16),
            vmem((2, rows, model), bf16),
            vmem((2, rows, model), bf16),
            vmem((n_mp,) + obs_mask.shape, jnp.int32),
            vmem((n_mp, slots, model), f32),
            vmem((2, n_mp, n_mp * slots, model), bf16),
            vmem((model, wide), bf16),
            vmem(raising.shape, bf16),
            vmem((n_mp, slots, model), f32),
            dma((units, n_dp, parts)),
            dma((units, n_dp, parts)),
            dma((units,)),
            dma((3, 3, chunks)),
            dma((3, 3, chunks)),
            dma((2, 3, chunks)),
            dma((2, 3, chunks)),
            dma((n_mp,)),
            dma((n_mp,)),
            dma((2, n_mp)),
            dma((2, n_mp)),
            dma((n_mp,)),
            dma((n_mp,)),
        ]
        + [vmem(weight.shape, weight.dtype) for weight in head_weights]
        + [vmem((model, n_dp * per_owner), bf16)]
        + [vmem((n_dp, per_owner, 3 * 128), bf16)] * 2
        + [vmem((n_dp, per_owner, model), bf16)] * 4
        + [dma((len(head_weights),))]
        + [dma((n_dp,))] * 6,
        compiler_params=pltpu.CompilerParams(collective_id=50, has_side_effects=True),
        name="trunk",
    )(
        tokens,
        obs_mask,
        norm_gains,
        attn_in,
        attn_out,
        raising,
        lowering,
        embodiment,
        levels,
        actions,
        noise,
        action_dims,
        *head_weights,
    )


def general_trunk(ident, tokens, obs_mask, norm_gains, attn_in, attn_out, mlp_in, mlp_out, small):
    model = tokens.shape[1]
    width = attn_in.shape[3]
    heads_local = width // HDIM
    samples_local, length = obs_mask.shape
    layer_count = attn_in.shape[0]
    n_mp = lax.axis_size("mp")
    samples_group = samples_local * n_mp
    joined = [
        jnp.concatenate(
            [attn_in[layer, 0], attn_in[layer, 1], attn_in[layer, 2], attn_out[layer].T], axis=1
        )
        for layer in range(layer_count)
    ]
    lowered = [mlp_out[layer].T for layer in range(layer_count)]


    residual = tokens.astype(jnp.float32)
    wide = None
    allowed = None
    mask_group = None
    got_small = None
    position = jnp.arange(length)
    for layer in range(layer_count):
        final = layer == layer_count - 1
        normed = normalize(residual, norm_gains[2 * layer]).astype(jnp.bfloat16)
        if layer == 0:
            sends = [("cast", normed), ("cast", obs_mask), ("swap", small), ("ring", joined[0])]
        else:
            sends = [("cast", normed)]
        if final:
            ends = residual.reshape(samples_local, length, model)[:, length - READ :, :]
            sends += [("cast", ends), ("ring", mlp_in[layer]), ("ring", lowered[layer])]
        got = list(exchange(next(ident), *sends))
        gathered = got.pop(0).reshape(-1, model)
        if layer == 0:
            mask_group = got.pop(0).reshape(samples_group, length)
            got_small = got.pop(0)
            wide = got.pop(0).reshape(model, -1)
            visible = (mask_group == 1) & (position < length - READ)[None, :]
            itself = position[:, None] == position[None, :]
            allowed = visible[:, None, :] | itself[None, :, :]
        if final:
            ends = got.pop(0).reshape(samples_group * READ, model)
            upper = got.pop(0).reshape(model, -1)
            lower = got.pop(0).reshape(model, -1)
            asking = gathered.reshape(samples_group, length, model)[:, length - READ :, :]
            queries = dot32(asking.reshape(-1, model), wide[:, :width]).astype(jnp.bfloat16)
            queries = queries.reshape(samples_group, READ, heads_local, HDIM)
            both = dot32(gathered, wide[:, width : 3 * width]).astype(jnp.bfloat16)
            keys_at = both[:, :width].reshape(samples_group, length, heads_local, HDIM)
            values_at = both[:, width:].reshape(samples_group, length, heads_local, HDIM)
            context = attend(queries, keys_at, values_at, allowed[:, length - READ :, :])
            partial_value = dot_turned(context.reshape(-1, width), wide[:, 3 * width :])
            (terms,) = exchange(next(ident), ("cast", partial_value.astype(jnp.bfloat16)))
            ends = ends + added(terms)
            normed = normalize(ends, norm_gains[2 * layer + 1]).astype(jnp.bfloat16)
            hidden = jax.nn.gelu(dot32(normed, upper), approximate=True).astype(jnp.bfloat16)
            partial_value = dot_turned(hidden, lower)
            (terms,) = exchange(next(ident), ("cast", partial_value.astype(jnp.bfloat16)))
            ends = ends + added(terms)
            break
        projected = dot32(gathered, wide[:, : 3 * width]).astype(jnp.bfloat16)
        split = [
            projected[:, part * width : (part + 1) * width].reshape(
                samples_group, length, heads_local, HDIM
            )
            for part in range(3)
        ]
        context = attend(split[0], split[1], split[2], allowed).reshape(-1, width)
        partial_value = dot_turned(context, wide[:, 3 * width :]).astype(jnp.bfloat16)
        terms, upper = exchange(
            next(ident),
            ("split", partial_value.reshape(n_mp, -1, model)),
            ("ring", mlp_in[layer]),
        )
        residual = residual + added(terms)
        normed = normalize(residual, norm_gains[2 * layer + 1]).astype(jnp.bfloat16)
        gathered, lower = exchange(next(ident), ("cast", normed), ("ring", lowered[layer]))
        raised = dot32(gathered.reshape(-1, model), upper.reshape(model, -1))
        hidden = jax.nn.gelu(raised, approximate=True).astype(jnp.bfloat16)
        partial_value = dot_turned(hidden, lower.reshape(model, -1)).astype(jnp.bfloat16)
        terms, wide = exchange(
            next(ident),
            ("split", partial_value.reshape(n_mp, -1, model)),
            ("ring", joined[layer + 1]),
        )
        wide = wide.reshape(model, -1)
        residual = residual + added(terms)

    return normalize(ends, norm_gains[2 * layer_count]).astype(jnp.bfloat16), got_small


def fused(
    tokens,
    obs_mask,
    norm_gains,
    attn_in,
    attn_out,
    mlp_in,
    mlp_out,
    embodiment,
    levels,
    actions,
    noise,
    action_dims,
    head_read,
    head_act,
    time_table,
    block_in,
    block_out,
    head_out,
):
    outs = trunk(
        tokens,
        obs_mask,
        norm_gains,
        attn_in,
        attn_out,
        mlp_in,
        jnp.swapaxes(mlp_out, 1, 2),
        embodiment.T,
        levels.T,
        actions,
        noise,
        action_dims,
        head_read,
        head_act,
        jnp.swapaxes(time_table, 0, 1),
        block_in,
        block_out,
        jnp.swapaxes(head_out, 1, 2),
    )
    back, read, act, times, inner, outer, final = outs
    return back, read, act, jnp.swapaxes(times, 0, 1), inner, outer, jnp.swapaxes(final, 1, 2)


def fits_fused(tokens, obs_mask, attn_in, mlp_in, head_read, actions):
    n_mp, n_dp = lax.axis_size("mp"), lax.axis_size("dp")
    model, width = tokens.shape[1], attn_in.shape[3]
    pad = model // 3 - width
    return (
        n_mp == 4
        and n_dp % 2 == 0
        and attn_in.shape[0] == 2
        and attn_in.shape[2] % 16 == 0
        and mlp_in.shape[2] == model
        and (model // 3) % 128 == 0
        and 3 * pad == width
        and tokens.shape[0] % CHUNK == 0
        and obs_mask.shape[1] == CHUNK
        and head_read.shape[0] * READ == 8
        and actions.shape[2] <= 128
    )


def on_device(
    tokens,
    obs_mask,
    norm_gains,
    attn_in,
    attn_out,
    mlp_in,
    mlp_out,
    embodiment,
    levels,
    actions,
    noise,
    action_dims,
    head_read,
    head_act,
    time_table,
    block_in,
    block_out,
    head_out,
):
    if fits_fused(tokens, obs_mask, attn_in, mlp_in, head_read, actions):
        return fused(
            tokens,
            obs_mask,
            norm_gains,
            attn_in,
            attn_out,
            mlp_in,
            mlp_out,
            embodiment,
            levels,
            actions,
            noise,
            action_dims,
            head_read,
            head_act,
            time_table,
            block_in,
            block_out,
            head_out,
        )
    model = tokens.shape[1]
    act = actions.shape[2]
    samples_local = obs_mask.shape[0]
    n_mp, n_dp = lax.axis_size("mp"), lax.axis_size("dp")
    my_model, my_owner = lax.axis_index("mp"), lax.axis_index("dp")
    samples_group = samples_local * n_mp
    ident = iter(range(100))

    heads_dev = head_read.shape[0]
    slot_count = heads_dev * n_dp
    owners = embodiment[:, 0]
    table = plan()
    onto = (jnp.arange(slot_count)[:, None] == owners[None, :]).astype(jnp.bfloat16)
    spread_rows = jnp.einsum("es,rq->ersq", onto, jnp.eye(READ, dtype=jnp.bfloat16)).reshape(
        slot_count * READ, samples_group * READ
    )
    small = jnp.concatenate(
        [
            noisy_pair(levels, actions, noise, table),
            noise,
            (levels + 1)[..., None].astype(jnp.bfloat16),
        ],
        axis=-1,
    ).reshape(samples_group * READ, 2 * act + 1)
    small = jnp.pad(small, ((0, 0), (0, -small.shape[1] % 128)))
    small = dot32(spread_rows, small).astype(jnp.bfloat16)
    small = small.reshape(n_dp, heads_dev * READ, small.shape[1])

    readouts, got_small = general_trunk(
        ident, tokens, obs_mask, norm_gains, attn_in, attn_out, mlp_in, mlp_out, small
    )
    send = dot32(spread_rows, readouts).astype(jnp.bfloat16)
    send = send.reshape(n_dp, heads_dev * READ, model)
    (got_features,) = exchange(next(ident), ("swap", send))

    def by_head(values):
        values = values.reshape(n_dp, heads_dev, READ, values.shape[-1])
        return jnp.moveaxis(values, 1, 0).reshape(heads_dev, n_dp * READ, values.shape[-1])

    head_features = by_head(got_features)
    head_small = by_head(got_small)
    head_noisy = head_small[..., :act]
    head_target = head_small[..., act : 2 * act].astype(jnp.float32)
    head_levels = head_small[..., 2 * act].astype(jnp.int32) - 1
    head_onehot = (head_levels[..., None] == jnp.arange(LEVELS)).astype(jnp.bfloat16)
    slot_ids = my_owner * heads_dev + jnp.arange(heads_dev)
    dims_here = jnp.sum(
        jnp.where(jnp.arange(EMB)[None, :] == slot_ids[:, None], action_dims[None, :], 0), axis=1
    )
    column = jnp.arange(act) % ADIM_MAX
    weight_mask = (head_levels >= 0).astype(jnp.float32)[..., None] * (
        column[None, None, :] < dims_here[:, None, None]
    ).astype(jnp.float32)
    others = jnp.einsum("hna,hac->hnc", head_noisy, head_act, preferred_element_type=jnp.float32)
    others = others + jnp.einsum(
        "hnl,hlc->hnc", head_onehot, time_table, preferred_element_type=jnp.float32
    )
    first = (
        jnp.einsum("hnd,hdc->hnc", head_features, head_read, preferred_element_type=jnp.float32)
        + others
    )
    grad_first, grad_inner, grad_outer, grad_final = jax.vmap(head_grads)(
        first,
        block_in.astype(jnp.float32),
        block_out.astype(jnp.float32),
        head_out.astype(jnp.float32),
        head_target,
        weight_mask,
    )
    grad_bf = grad_first.astype(jnp.bfloat16)
    backward = jnp.einsum(
        "hnc,hdc->hnd", grad_bf, head_read, preferred_element_type=jnp.float32
    ).astype(jnp.bfloat16)
    backward = jnp.moveaxis(backward.reshape(heads_dev, n_dp, READ, model), 0, 1)
    (arrived,) = exchange(
        next(ident), ("swap", backward.reshape(n_dp, heads_dev * READ, model))
    )
    mine = lax.dynamic_slice_in_dim(
        spread_rows, my_model * (samples_local * READ), samples_local * READ, 1
    )
    returned = lax.dot_general(
        mine,
        arrived.reshape(slot_count * READ, model),
        (((0,), (0,)), ((), ())),
        preferred_element_type=jnp.float32,
    ).astype(jnp.bfloat16)
    feature_width = model // n_mp
    own_features = lax.dynamic_slice_in_dim(
        head_features, my_model * feature_width, feature_width, 2
    )
    grad_readin = jnp.einsum(
        "hnd,hnc->hdc", own_features, grad_bf, preferred_element_type=jnp.float32
    )
    grad_actin = jnp.einsum("hna,hnc->hac", head_noisy, grad_bf, preferred_element_type=jnp.float32)
    grad_timein = jnp.einsum(
        "hnl,hnc->hlc", head_onehot, grad_bf, preferred_element_type=jnp.float32
    )
    return (
        returned.reshape(samples_local, READ, model),
        grad_readin,
        grad_actin,
        grad_timein,
        grad_inner,
        grad_outer,
        grad_final,
    )


def solution(mesh):
    placed = (
        P(("dp", "mp"), None),
        P(("dp", "mp"), None),
        P(),
        P(None, None, "dp", "mp"),
        P(None, "mp", "dp"),
        P(None, "dp", "mp"),
        P(None, "mp", "dp"),
        P("dp", None),
        P("dp", None),
        P("dp", None, None),
        P("dp", None, None),
        P(),
        P("dp", None, None),
        P("dp", None, None),
        P("dp", None, None),
        P("dp", None, None),
        P("dp", None, None),
        P("dp", None, None),
    )
    return jax.shard_map(
        on_device,
        mesh=mesh,
        in_specs=placed,
        out_specs=(
            P(("dp", "mp"), None, None),
            P("dp", "mp", None),
            P("dp", None, None),
            P("dp", None, None),
            P("dp", None, None),
            P("dp", None, None),
            P("dp", None, None),
        ),
        check_vma=False,
    )
```

```python
import functools
import math

import jax
import jax.numpy as jnp
from jax import lax
from jax.experimental import pallas as pl
from jax.experimental.pallas import tpu as pltpu
from jax.sharding import PartitionSpec as P

HDIM = 64
EMB = 25
READ = 2
LEVELS = 20
ADIM_MAX = 14

norm_eps = 1e-05
MESH_ID = pl.DeviceIdType.MESH


def normalize(values, scale_gain):
    center = values - jnp.mean(values, axis=-1, keepdims=True)
    spread = jnp.mean(center * center, axis=-1, keepdims=True)
    return center * lax.rsqrt(spread + norm_eps) * scale_gain


def plan():
    steps_up = (jnp.arange(LEVELS, dtype=jnp.float32) + 1.0) / LEVELS
    anchor = math.cos(0.008 / 1.008 * math.pi / 2) ** 2
    return jnp.cos((steps_up + 0.008) / 1.008 * (math.pi / 2)) ** 2 / anchor


def noisy_pair(level_ids, clean, noise_draw, table):
    picked = (level_ids[..., None] == jnp.arange(LEVELS)).astype(jnp.float32)
    kept = jnp.sum(picked * table, axis=-1)[..., None]
    mixed = jnp.sqrt(kept) * clean.astype(jnp.float32) + jnp.sqrt(1.0 - kept) * noise_draw.astype(
        jnp.float32
    )
    return mixed.astype(jnp.bfloat16)


def ring_place(index, size):
    if size % 2:
        return index
    odd = index % 2
    return (1 - odd) * (index // 2) + odd * (size - 1 - index // 2)


def ring_index(place, size):
    if size % 2:
        return place
    back = place // (size // 2)
    return (1 - back) * (2 * place) + back * (2 * (size - 1 - place) + 1)


def ring_parts(rows, tile=16):
    if rows % tile:
        return [(0, rows)]
    return [(start, tile) for start in range(0, rows, tile)]


def ring_step(parts, step, size):
    count = len(parts)
    if size % 2 == 0 and step == size // 2 - 1:
        near = (count + 1) // 2
        pairs = [(0, chunk) for chunk in range(near)], [(1, chunk) for chunk in range(near, count)]
        mixed = []
        for chunk in range(near):
            mixed += [side[chunk] for side in pairs if chunk < len(side)]
        return mixed
    return [(way, chunk) for chunk in range(count) for way in range(2)]


def exchange_kernel(n_dp, n_mp, kinds, *refs):
    count = len(kinds)
    ins, outs = refs[:count], refs[count : 2 * count]
    sems = refs[2 * count :]
    local_sem = sems[-1]
    my_dp, my_mp = lax.axis_index("dp"), lax.axis_index("mp")
    place = ring_place(my_dp, n_dp)

    talk_mp = any(kind in ("split", "cast") for kind in kinds)
    talk_dp = "swap" in kinds
    talk_ring = "ring" in kinds
    barrier = pltpu.get_barrier_semaphore()
    greeted = 0
    if talk_mp:
        for offset in range(1, n_mp):
            pl.semaphore_signal(
                barrier, inc=1, device_id={"mp": (my_mp + offset) % n_mp}, device_id_type=MESH_ID
            )
            greeted += 1
    if talk_dp:
        for offset in range(1, n_dp):
            pl.semaphore_signal(
                barrier, inc=1, device_id={"dp": (my_dp + offset) % n_dp}, device_id_type=MESH_ID
            )
            greeted += 1
    elif talk_ring:
        for way in (1, n_dp - 1):
            pl.semaphore_signal(
                barrier,
                inc=1,
                device_id={"dp": ring_index((place + way) % n_dp, n_dp)},
                device_id_type=MESH_ID,
            )
            greeted += 1
    pl.semaphore_wait(barrier, greeted)

    def ring_copies(item, step):
        source, landing = ins[item], outs[item]
        parts = ring_parts(source.shape[0])
        made = {}
        for way, chunk in ring_step(parts, step, n_dp):
            origin = ring_index((place + (n_dp - step if way == 0 else step)) % n_dp, n_dp)
            target = ring_index((place + (1 if way == 0 else n_dp - 1)) % n_dp, n_dp)
            rows = pl.ds(*parts[chunk])
            spot = landing.at[origin, rows]
            made[way, chunk] = pltpu.make_async_remote_copy(
                src_ref=source.at[rows] if step == 0 else spot,
                dst_ref=spot,
                send_sem=sems[2 * item].at[step, chunk, way],
                recv_sem=sems[2 * item + 1].at[step, chunk, way],
                device_id={"dp": target},
                device_id_type=MESH_ID,
            )
        return made

    rings = [item for item in range(count) if kinds[item] == "ring"]
    flights = {item: ring_copies(item, 0) for item in rings}
    for item in rings:
        for copy in flights[item].values():
            copy.start()
    direct = []
    keeps = []
    for item, kind in enumerate(kinds):
        source, landing = ins[item], outs[item]
        if kind == "ring":
            keeps.append(pltpu.make_async_copy(source, landing.at[my_dp], local_sem.at[item]))
            continue
        size, mine, axis = (n_dp, my_dp, "dp") if kind == "swap" else (n_mp, my_mp, "mp")
        for offset in range(1, size):
            peer = (mine + offset) % size
            copy = pltpu.make_async_remote_copy(
                src_ref=source if kind == "cast" else source.at[peer],
                dst_ref=landing.at[mine],
                send_sem=sems[2 * item].at[offset],
                recv_sem=sems[2 * item + 1].at[offset],
                device_id={axis: peer},
                device_id_type=MESH_ID,
            )
            copy.start()
            direct.append(copy)
        keeps.append(
            pltpu.make_async_copy(
                source if kind == "cast" else source.at[mine], landing.at[mine], local_sem.at[item]
            )
        )
    for keep in keeps:
        keep.start()
    sent = [copy for item in rings for copy in flights[item].values()]
    landed = []
    for step in range(1, n_dp // 2):
        for item in rings:
            following = ring_copies(item, step)
            for key, after in following.items():
                flights[item].pop(key).wait_recv()
                after.start()
            landed += flights[item].values()
            flights[item] = following
            sent += following.values()
    for item in rings:
        landed += flights[item].values()
    for copy in landed:
        copy.wait_recv()
    for copy in direct:
        copy.wait_recv()
    for copy in sent + direct:
        copy.wait_send()
    for keep in keeps:
        keep.wait()


def exchange(ident, *pairs):
    n_dp, n_mp = lax.axis_size("dp"), lax.axis_size("mp")
    kinds = tuple(kind for kind, _ in pairs)
    arrays = [array for _, array in pairs]
    shapes, scratch = [], []
    for kind, array in pairs:
        lead = {"ring": (n_dp,), "cast": (n_mp,), "split": (), "swap": ()}[kind]
        shapes.append(jax.ShapeDtypeStruct(lead + array.shape, array.dtype))
        if kind == "ring":
            slots = (n_dp // 2, len(ring_parts(array.shape[0])), 2)
        else:
            slots = (n_dp if kind == "swap" else n_mp,)
        scratch += [pltpu.SemaphoreType.DMA(slots), pltpu.SemaphoreType.DMA(slots)]
    scratch.append(pltpu.SemaphoreType.DMA((len(pairs),)))
    return pl.pallas_call(
        functools.partial(exchange_kernel, n_dp, n_mp, kinds),
        out_shape=shapes,
        in_specs=[pl.BlockSpec(memory_space=pltpu.VMEM)] * len(pairs),
        out_specs=[pl.BlockSpec(memory_space=pltpu.VMEM)] * len(pairs),
        scratch_shapes=scratch,
        compiler_params=pltpu.CompilerParams(collective_id=ident, has_side_effects=True),
        name="exchange%d" % ident,
    )(*arrays)


def attend(queries, key_rows, value_rows, allowed):
    scores = jnp.einsum(
        "sqhd,skhd->shqk", queries, key_rows, preferred_element_type=jnp.float32
    ) * HDIM ** (-0.5)
    weights = jnp.where(allowed[:, None, :, :], jnp.exp(scores), 0.0)
    shares = (weights / jnp.sum(weights, axis=-1, keepdims=True)).astype(jnp.bfloat16)
    context = jnp.einsum("shqk,skhd->sqhd", shares, value_rows, preferred_element_type=jnp.float32)
    return context.astype(jnp.bfloat16)


def dot32(left, right):
    return jnp.dot(left, right, preferred_element_type=jnp.float32)


def dot_turned(left, right):
    return lax.dot_general(
        left, right, (((1,), (1,)), ((), ())), preferred_element_type=jnp.float32
    )


def added(blocks):
    return jnp.sum(blocks.astype(jnp.float32), axis=0)


def tail(first, target, weight_mask, inner_weight, outer_weight, final_weight):
    highest = lax.Precision.HIGHEST
    active = jax.nn.silu(first).astype(jnp.bfloat16)
    inner = jnp.dot(active, inner_weight, preferred_element_type=jnp.float32, precision=highest)
    second = jax.nn.silu(inner).astype(jnp.bfloat16)
    hidden = first + jnp.dot(
        second, outer_weight, preferred_element_type=jnp.float32, precision=highest
    )
    third = jax.nn.silu(hidden).astype(jnp.bfloat16)
    predicted = jnp.dot(third, final_weight, preferred_element_type=jnp.float32, precision=highest)
    differ = predicted - target
    return 0.5 * jnp.sum(weight_mask * differ * differ)


def head_grads(first, inner_weight, outer_weight, final_weight, target, weight_mask):

    def head_loss(first_in, inner_in, outer_in, final_in):
        return tail(first_in, target, weight_mask, inner_in, outer_in, final_in)

    loss_value, pullback = jax.vjp(head_loss, first, inner_weight, outer_weight, final_weight)
    return pullback(jnp.ones((), jnp.float32))


CHUNK = 64
RING_STARTS = (0, 2, 4, 5, 6, 7)
RING_PARTS = 2
PUMPS = (1, 1, 2, 2, 7, 7, 9, 9, 10, 13, 13, 14, 14, 16, 17, 17, 18, 20, 21, 22, 23, 23, 24, 25, 26, 27, 27, 28, 29)


def remote(source, landing, send_sem, recv_sem, where):
    return pltpu.make_async_remote_copy(
        src_ref=source,
        dst_ref=landing,
        send_sem=send_sem,
        recv_sem=recv_sem,
        device_id=where,
        device_id_type=MESH_ID,
    )


def trunk_kernel(
    n_dp,
    n_mp,
    tokens,
    obs_mask,
    norm_gains,
    attn_in,
    attn_out,
    raising,
    lowering,
    embodiment,
    levels,
    actions,
    noise,
    action_dims,
    read_hbm,
    act_hbm,
    time_hbm,
    inner_hbm,
    outer_hbm,
    final_hbm,
    back_out,
    read_out,
    act_out,
    time_out,
    inner_out,
    outer_out,
    final_out,
    full,
    cast_rows,
    residual,
    projected,
    context,
    hidden,
    partial_rows,
    near_part,
    far_part,
    own_part,
    paired,
    mask_all,
    ends_all,
    end_terms,
    out_weight,
    joined,
    returned,
    ring_send,
    ring_recv,
    keep_sem,
    cast_send,
    cast_recv,
    sum_send,
    sum_recv,
    ends_send,
    ends_recv,
    term_send,
    term_recv,
    mask_send,
    mask_recv,
    read_w,
    act_w,
    time_w,
    inner_w,
    outer_w,
    final_w,
    turned,
    small_out,
    small_in,
    rows_out,
    rows_in,
    back_rows,
    back_in,
    weight_sem,
    small_send,
    small_recv,
    rows_send,
    rows_recv,
    back_send,
    back_recv,
):
    layer_count = joined.shape[0]
    rows, model = residual.shape
    block = joined.shape[1]
    samples, length = obs_mask.shape
    width = model // n_mp
    wide = model // 3
    pad = wide - width
    heads = width // HDIM
    chunks = rows // CHUNK
    parts = ring_send.shape[2]
    f32, bf16 = jnp.float32, jnp.bfloat16

    my_dp, my_mp = lax.axis_index("dp"), lax.axis_index("mp")
    core = my_mp % 2
    sib = my_mp + 1 - 2 * core
    far = (my_mp + 2) % n_mp
    far_sib = (sib + 2) % n_mp
    sib_id, far_id = {"mp": sib}, {"mp": far}

    barrier = pltpu.get_barrier_semaphore()
    for offset in range(1, n_mp):
        pl.semaphore_signal(
            barrier, inc=1, device_id={"mp": (my_mp + offset) % n_mp}, device_id_type=MESH_ID
        )
    for offset in range(1, n_dp):
        pl.semaphore_signal(
            barrier, inc=1, device_id={"dp": (my_dp + offset) % n_dp}, device_id_type=MESH_ID
        )

    def gain(index):
        return norm_gains[index : index + 1, :]

    def norm_chunk(index, chunk, gain_index):
        at = pl.ds(chunk * CHUNK, CHUNK)
        cast_rows[index, my_mp, at, :] = normalize(residual[at, :], gain(gain_index)).astype(bf16)

    def flipped(left, right):
        return lax.dot_general(
            left, right, (((0,), (0,)), ((), ())), preferred_element_type=f32
        )

    piece_row = lax.broadcasted_iota(jnp.int32, (width, model), 0)
    piece_lane = lax.broadcasted_iota(jnp.int32, (width, model), 1)
    picks = piece_lane == (piece_row // pad) * wide + width + piece_row % pad
    placing = jnp.where(picks, 1.0, 0.0).astype(bf16)

    def join(layer):
        joined[layer] = flipped(attn_out[layer], placing).astype(bf16)
        for part in range(3):
            joined[layer, :, part * wide : part * wide + width] = attn_in[layer, part]

    join(0)
    for chunk in range(chunks):
        at = pl.ds(chunk * CHUNK, CHUNK)
        residual[at, :] = tokens[at, :].astype(f32)
        norm_chunk(0, chunk, 0)
    mask_all[my_mp] = obs_mask[...]
    pl.semaphore_wait(barrier, n_mp + n_dp - 2)

    sources = [part.at[layer] for layer in range(layer_count) for part in (joined, raising, lowering)]

    place = ring_place(my_dp, n_dp)
    half = n_dp // 2
    piece = block // parts

    def spot(unit, origin, part):
        return full.at[unit, pl.ds(pl.multiple_of(origin * block + part * piece, 16), piece)]

    def hop(unit, step, way, part):
        origin = ring_index((place + (n_dp - step if way == 0 else step)) % n_dp, n_dp)
        target = ring_index((place + (1 if way == 0 else n_dp - 1)) % n_dp, n_dp)
        here = spot(unit, origin, part)
        slot = step * 2 + way
        return remote(
            sources[unit].at[pl.ds(part * piece, piece)] if step == 0 else here,
            here,
            ring_send.at[unit, slot, part],
            ring_recv.at[unit, slot, part],
            {"dp": target},
        )

    def landed(unit, step, way, part):
        origin = ring_index(
            (place + (n_dp - step - 1 if way == 0 else step + 1)) % n_dp, n_dp
        )
        here = spot(unit, origin, part)
        slot = step * 2 + way
        return remote(
            here,
            here,
            ring_send.at[unit, slot, part],
            ring_recv.at[unit, slot, part],
            {"dp": ring_index((place + (1 if way == 0 else n_dp - 1)) % n_dp, n_dp)},
        )

    def legs(step):
        return [
            (way, part)
            for part in range(parts)
            for way in range(2)
            if step < half - 1 or (part < (parts + 1) // 2) == (way == 0)
        ]

    def kept(unit):
        return pltpu.make_async_copy(
            sources[unit],
            full.at[unit, pl.ds(pl.multiple_of(my_dp * block, block), block)],
            keep_sem.at[unit],
        )

    events = sorted(
        (RING_STARTS[unit] + step, unit, step)
        for unit in range(len(sources))
        for step in range(half + 1)
    )
    done = [0]

    def pump(count):
        while done[0] < min(count, len(events)):
            _, unit, step = events[done[0]]
            done[0] += 1
            if step == 0:
                for way, part in legs(0):
                    hop(unit, 0, way, part).start()
                kept(unit).start()
                continue
            after = legs(step) if step < half else []
            for way, part in legs(step - 1):
                landed(unit, step - 1, way, part).wait_recv()
                if (way, part) in after:
                    hop(unit, step, way, part).start()

    def complete(unit):
        pump(events.index((RING_STARTS[unit] + half, unit, half)) + 1)
        kept(unit).wait()

    def cast_copy(index, way, chunk):
        at = pl.ds(chunk * CHUNK, CHUNK)
        whose = far if way == 2 else my_mp
        place = cast_rows.at[index, whose, at]
        return remote(
            place,
            place,
            cast_send.at[index, way, chunk],
            cast_recv.at[index, way, chunk],
            far_id if way == 1 else sib_id,
        )

    def cast_landed(index, way, chunk):
        at = pl.ds(chunk * CHUNK, CHUNK)
        place = cast_rows.at[index, (sib, far, far_sib)[way], at]
        return remote(
            place,
            place,
            cast_send.at[index, way, chunk],
            cast_recv.at[index, way, chunk],
            far_id if way == 1 else sib_id,
        )

    def cast_pass(index, chunk):
        cast_landed(index, 1, chunk).wait_recv()
        cast_copy(index, 2, chunk).start()

    def cast_near(index):
        for chunk in range(chunks):
            cast_landed(index, 0, chunk).wait_recv()

    def cast_far(index):
        for chunk in range(chunks):
            cast_landed(index, 2, chunk).wait_recv()

    def sum_near(index):
        return remote(
            partial_rows.at[far_sib],
            near_part.at[index],
            sum_send.at[index, 0, 0],
            sum_recv.at[index, 0, 0],
            sib_id,
        )

    def sum_own(index):
        return remote(
            partial_rows.at[sib],
            own_part.at[index],
            sum_send.at[index, 1, 0],
            sum_recv.at[index, 1, 0],
            sib_id,
        )

    def sum_far(index, chunk):
        at = pl.ds(chunk * CHUNK, CHUNK)
        return remote(
            paired.at[index, at],
            far_part.at[index, at],
            sum_send.at[index, 2, chunk],
            sum_recv.at[index, 2, chunk],
            far_id,
        )

    def sum_cross(index):
        sum_near(index).wait_recv()
        for chunk in range(chunks):
            at = pl.ds(chunk * CHUNK, CHUNK)
            paired[index, at, :] = (
                partial_rows[far, at, :].astype(f32) + near_part[index, at, :].astype(f32)
            ).astype(bf16)
            sum_far(index, chunk).start()

    def sum_finish(index, next_cast, gain_index):
        sum_own(index).wait_recv()
        for chunk in range(chunks):
            at = pl.ds(chunk * CHUNK, CHUNK)
            sum_far(index, chunk).wait_recv()
            residual[at, :] = (
                residual[at, :]
                + own_part[index, at, :].astype(f32)
                + far_part[index, at, :].astype(f32)
            )
            norm_chunk(next_cast, chunk, gain_index)
            cast_copy(next_cast, 1, chunk).start()
            cast_copy(next_cast, 0, chunk).start()
            pump(PUMPS[(9, 19)[index] + chunk])

    def peers():
        return [(offset, {"mp": (my_mp + offset) % n_mp}) for offset in range(1, n_mp)]

    def ends_copy(offset, who):
        return remote(
            ends_all.at[my_mp], ends_all.at[my_mp], ends_send.at[offset], ends_recv.at[offset], who
        )

    def term_copy(index, offset, who):
        place = end_terms.at[index, my_mp]
        return remote(place, place, term_send.at[index, offset], term_recv.at[index, offset], who)

    def term_landed(index, offset):
        place = end_terms.at[index, (my_mp + n_mp - offset) % n_mp]
        return remote(
            place, place, term_send.at[index, offset], term_recv.at[index, offset], sib_id
        )

    def mask_copy(offset, who):
        return remote(
            obs_mask, mask_all.at[my_mp], mask_send.at[offset], mask_recv.at[offset], who
        )

    def swap_copy(source, landing, send_sem, recv_sem, offset):
        peer = (my_dp + offset) % n_dp
        return remote(
            source.at[peer],
            landing.at[my_dp],
            send_sem.at[offset],
            recv_sem.at[offset],
            {"dp": peer},
        )

    def swap_landed(source, landing, send_sem, recv_sem, offset):
        peer = (my_dp + n_dp - offset) % n_dp
        return remote(
            source.at[peer],
            landing.at[peer],
            send_sem.at[offset],
            recv_sem.at[offset],
            {"dp": peer},
        )

    def swap_start(*swap):
        for offset in range(1, n_dp):
            swap_copy(*swap, offset).start()
        swap[1][my_dp] = swap[0][my_dp]

    def swap_wait(*swap):
        for offset in range(1, n_dp):
            swap_landed(*swap, offset).wait_recv()

    small_swap = (small_out, small_in, small_send, small_recv)
    rows_swap = (rows_out, rows_in, rows_send, rows_recv)
    back_swap = (back_rows, back_in, back_send, back_recv)
    head_count, slot_rows = read_hbm.shape[0], rows_in.shape[1]
    all_rows = n_dp * slot_rows
    weight_copies = [
        pltpu.make_async_copy(source, landing, weight_sem.at[index])
        for index, (source, landing) in enumerate(
            (
                (read_hbm, read_w),
                (act_hbm, act_w),
                (time_hbm, time_w),
                (inner_hbm, inner_w),
                (outer_hbm, outer_w),
                (final_hbm, final_w),
            )
        )
    ]

    pump(PUMPS[0])
    for offset, who in peers():
        mask_copy(offset, who).start()
    for chunk in range(chunks):
        cast_copy(0, 1, chunk).start()
        cast_copy(0, 0, chunk).start()
    for copy in weight_copies:
        copy.start()
    join(1)
    group = levels.shape[1]
    act = actions.shape[2]
    tile = 128
    slots = ends_all.shape[1]
    end_rows = n_mp * slots
    slot_of = lax.broadcasted_iota(jnp.int32, (all_rows, group), 0)
    sample_at = lax.broadcasted_iota(jnp.int32, (group, end_rows), 0)
    end_of = lax.broadcasted_iota(jnp.int32, (group, end_rows), 1)
    end_sample = (end_of // slots) * samples + end_of % slots // READ
    end_here = (end_sample == sample_at) & (end_of % slots < samples * READ)
    square = lax.broadcasted_iota(jnp.int32, (group, group), 0)
    square = square == lax.broadcasted_iota(jnp.int32, (group, group), 1)
    level_lane = lax.broadcasted_iota(jnp.int32, (group, tile), 1)
    table_lane = lax.broadcasted_iota(jnp.int32, (1, tile), 1)
    table = jnp.zeros((1, tile), f32)
    for level, value in enumerate(plan_values()):
        table = jnp.where(table_lane == level, value, table)
    spread = jnp.zeros((all_rows, end_rows), f32)
    scattered = [jnp.zeros((all_rows, act), f32)] * 2 + [jnp.zeros((all_rows, tile), f32)]
    clean_all, noise_all = actions[...].astype(f32), noise[...].astype(f32)
    for read in range(READ):
        route = (embodiment[...] == slot_of // READ) & (slot_of % READ == read)
        route = jnp.where(route, 1.0, 0.0).astype(bf16)
        ends_here = jnp.where(end_here & (end_of % READ == read), 1.0, 0.0).astype(bf16)
        spread = spread + dot32(route, ends_here)
        level = jnp.sum(
            jnp.where(square, levels[read : read + 1, :], 0), axis=1, keepdims=True
        )
        onehot = jnp.where(level_lane == level, 1.0, 0.0)
        kept_share = jnp.sum(onehot * table, axis=1, keepdims=True)
        clean, drawn = clean_all[:, read, :], noise_all[:, read, :]
        mixed = jnp.sqrt(kept_share) * clean + jnp.sqrt(1.0 - kept_share) * drawn
        for index, values in enumerate((mixed, drawn, onehot)):
            scattered[index] = scattered[index] + dot32(route, values.astype(bf16))
    spread = spread.astype(bf16)
    small_out[...] = jnp.zeros(small_out.shape, bf16)
    for peer in range(n_dp):
        at = slice(peer * slot_rows, (peer + 1) * slot_rows)
        for index, values in enumerate(scattered):
            columns = slice(index * tile, index * tile + values.shape[1])
            small_out[peer, :, columns] = values[at].astype(bf16)
    swap_start(*small_swap)
    for chunk in range(chunks):
        cast_pass(0, chunk)
        pump(PUMPS[1 + chunk])

    lane = lax.broadcasted_iota(jnp.int32, (1, wide), 1)
    lane_masks = [
        jnp.where((lane >= head * HDIM) & (lane < (head + 1) * HDIM), 1.0, 0.0).astype(f32)
        for head in range(heads)
    ]

    def take_out_weight(unit):
        row = lax.broadcasted_iota(jnp.int32, (model, wide), 0)
        spot_lane = lax.broadcasted_iota(jnp.int32, (model, wide), 1)
        picks = (row % wide >= width) & (spot_lane == (row // wide) * pad + row % wide - width)
        choose = jnp.where(picks, 1.0, 0.0).astype(bf16)
        out_weight[...] = dot32(full[unit], choose).astype(bf16)

    def pair_rows(first, body):
        def step(index, carry):
            body(first + index)
            return carry

        lax.fori_loop(0, 2, step, 0)

    near_first = my_mp - core
    far_first = (near_first + 2) % n_mp

    def project(index, unit, owner):
        at = pl.ds(pl.multiple_of(owner * rows, rows), rows)
        projected[at, :] = dot32(cast_rows[index, owner], full[unit]).astype(bf16)

    def attention(tail_rows):
        asked = tail_rows if tail_rows else length
        row = lax.broadcasted_iota(jnp.int32, (heads * asked, length), 0) % asked
        col = lax.broadcasted_iota(jnp.int32, (heads * asked, length), 1)
        itself = jnp.where(row + (length - asked) == col, 1.0, 0.0)
        narrow = lax.broadcasted_iota(jnp.int32, (1, length), 1)

        def step(owner, carry):
            for sample in range(samples):
                start = owner * rows + sample * length
                at = pl.ds(pl.multiple_of(start, length), length)
                ask = pl.ds(pl.multiple_of(start + length - asked, 16), asked)
                query = projected[ask, :wide].astype(f32) * HDIM ** (-0.5)
                stacked = jnp.concatenate(
                    [(query * lanes).astype(bf16) for lanes in lane_masks], axis=0
                )
                scores = dot_turned(stacked, projected[at, wide : 2 * wide])
                seen = mask_all[owner, sample : sample + 1, :]
                seen = jnp.where((seen == 1) & (narrow < length - READ), 1.0, 0.0)
                weights = jnp.where(jnp.maximum(itself, seen) > 0.0, jnp.exp(scores), 0.0)
                shares = (weights / jnp.sum(weights, axis=-1, keepdims=True)).astype(bf16)
                mixed = dot32(shares, projected[at, 2 * wide :])
                total = mixed[:asked] * lane_masks[0]
                for head in range(1, heads):
                    total = total + mixed[head * asked : (head + 1) * asked] * lane_masks[head]
                put = pl.ds(
                    pl.multiple_of(owner * (samples * asked) + sample * asked, 16), asked
                )
                context[put, :] = total.astype(bf16)
            return carry

        lax.fori_loop(0, n_mp, step, 0)

    def combine(index, part_of, late):
        if index:
            sum_near(index - 1).wait_send()
            sum_own(index - 1).wait_send()
        partial_rows[far_sib] = part_of(far_sib).astype(bf16)
        sum_near(index).start()
        partial_rows[far] = part_of(far).astype(bf16)
        partial_rows[sib] = part_of(sib).astype(bf16)
        sum_own(index).start()
        pump(PUMPS[(7, 17)[index]])
        sum_cross(index)
        residual[...] = residual[...] + part_of(my_mp)
        late()

    complete(0)
    cast_near(0)
    cast_far(0)
    for offset, who in peers():
        mask_copy(offset, who).wait_recv()
    take_out_weight(0)
    pair_rows(near_first, lambda owner: project(0, 0, owner))
    pump(PUMPS[4])
    pair_rows(far_first, lambda owner: project(0, 0, owner))
    pump(PUMPS[5])
    attention(0)
    pump(PUMPS[6])

    def attended(owner):
        at = pl.ds(pl.multiple_of(owner * rows, rows), rows)
        return dot_turned(context[at, :], out_weight[...])

    def after_attention():
        pump(PUMPS[8])

    combine(0, attended, after_attention)
    sum_finish(0, 1, 1)
    for chunk in range(chunks):
        cast_pass(1, chunk)
        pump(PUMPS[12 + chunk])
    complete(1)

    def raise_rows(owner):
        hidden[owner] = jax.nn.gelu(dot32(cast_rows[1, owner], full[1]), approximate=True).astype(
            bf16
        )

    cast_near(1)
    pair_rows(near_first, raise_rows)
    pump(PUMPS[15])
    cast_far(1)
    pair_rows(far_first, raise_rows)
    pump(PUMPS[16])
    complete(2)

    def lowered_rows(owner):
        return dot_turned(hidden[owner], full[2])

    def after_mlp():
        pump(PUMPS[18])

    combine(1, lowered_rows, after_mlp)
    sum_finish(1, 2, 2)
    ends_all[my_mp] = jnp.zeros(ends_all.shape[1:], f32)
    for sample in range(samples):
        last = (sample + 1) * length
        ends_all[my_mp, READ * sample : READ * (sample + 1), :] = residual[last - READ : last, :]
    for offset, who in peers():
        ends_copy(offset, who).start()
    for chunk in range(chunks):
        cast_pass(2, chunk)
        pump(PUMPS[22 + chunk])
    complete(3)
    take_out_weight(3)
    cast_near(2)
    pair_rows(near_first, lambda owner: project(2, 3, owner))
    pump(PUMPS[25])
    cast_far(2)
    pair_rows(far_first, lambda owner: project(2, 3, owner))
    pump(PUMPS[26])
    attention(16)
    pump(PUMPS[27])

    row = lax.broadcasted_iota(jnp.int32, (n_mp * slots, n_mp * samples * 16), 0)
    col = lax.broadcasted_iota(jnp.int32, (n_mp * slots, n_mp * samples * 16), 1)
    inner = row % slots
    wanted = ((row // slots) * samples + inner // READ) * 16 + 16 - READ + inner % READ
    choose = jnp.where((wanted == col) & (inner < samples * READ), 1.0, 0.0).astype(bf16)
    ends_context = dot32(choose, context[: n_mp * samples * 16, :]).astype(bf16)

    def share(index, value):
        end_terms[index, my_mp] = value.astype(bf16)
        for offset, who in peers():
            term_copy(index, offset, who).start()

    def gathered_terms(index, ends):
        for offset in range(1, n_mp):
            term_landed(index, offset).wait_recv()
        for owner in range(n_mp):
            ends = ends + end_terms[index, owner].astype(f32)
        return ends

    share(0, dot_turned(ends_context, out_weight[...]))
    pump(PUMPS[28])
    for offset, who in peers():
        remote(
            ends_all.at[my_mp],
            ends_all.at[(my_mp + n_mp - offset) % n_mp],
            ends_send.at[offset],
            ends_recv.at[offset],
            who,
        ).wait_recv()
    ends = jnp.concatenate([ends_all[owner] for owner in range(n_mp)], axis=0)
    ends = gathered_terms(0, ends)
    normed = normalize(ends, gain(3)).astype(bf16)
    complete(4)
    raised = jax.nn.gelu(dot32(normed, full[4]), approximate=True).astype(bf16)
    complete(5)
    share(1, dot_turned(raised, full[5]))
    ends = gathered_terms(1, ends)
    readouts = normalize(ends, gain(4)).astype(bf16)

    scattered = dot32(spread, readouts)
    for peer in range(n_dp):
        rows_out[peer] = scattered[peer * slot_rows : (peer + 1) * slot_rows].astype(bf16)
    swap_start(*rows_swap)
    for copy in weight_copies:
        copy.wait()
    swap_wait(*small_swap)
    facts = jnp.concatenate([small_in[peer].astype(f32) for peer in range(n_dp)], axis=0)
    noisy = facts[:, :tile].astype(bf16)
    target = facts[:, tile : tile + act]
    onehot = facts[:, 2 * tile :].astype(bf16)
    row_of = lax.broadcasted_iota(jnp.int32, (all_rows, act), 0) % slot_rows // READ
    live = jnp.sum(facts[:, 2 * tile :], axis=1, keepdims=True)
    column = lax.broadcasted_iota(jnp.int32, (1, act), 1) % ADIM_MAX
    times = time_w[...].astype(f32)
    firsts = [
        dot32(noisy[:, :act], act_w[head]) + dot32(onehot[:, :LEVELS], times[:, head, :].astype(bf16))
        for head in range(head_count)
    ]
    swap_wait(*rows_swap)
    features = jnp.concatenate([rows_in[peer].astype(f32) for peer in range(n_dp)], axis=0)
    features = features.astype(bf16)

    def slope(value):
        gate = jax.nn.sigmoid(value)
        return gate * (1.0 + value * (1.0 - gate))

    kept_back = []
    backward = jnp.zeros((all_rows, model), f32)
    for head in range(head_count):
        first = firsts[head] + dot32(features, read_w[head])
        active = jax.nn.silu(first).astype(bf16)
        inner = dot32(active, inner_w[head])
        second = jax.nn.silu(inner).astype(bf16)
        above = first + dot32(second, outer_w[head])
        third = jax.nn.silu(above).astype(bf16)
        predicted = dot_turned(third, final_w[head])
        slot = my_dp * head_count + head
        dims = jnp.where(slot < EMB, action_dims[jnp.minimum(slot, EMB - 1)], 0)
        mask = jnp.where((row_of == head) & (column < dims), live, 0.0)
        differ = (mask * (predicted - target)).astype(bf16)
        above_grad = dot32(differ, final_w[head]).astype(bf16).astype(f32) * slope(above)
        above_bf = above_grad.astype(bf16)
        inner_grad = dot_turned(above_bf, outer_w[head]).astype(bf16).astype(f32) * slope(inner)
        inner_bf = inner_grad.astype(bf16)
        first_grad = above_grad + dot_turned(inner_bf, inner_w[head]).astype(bf16).astype(
            f32
        ) * slope(first)
        first_bf = first_grad.astype(bf16)
        backward = backward + dot_turned(first_bf, read_w[head])
        kept_back.append((active, second, third, differ, above_bf, inner_bf, first_bf))
    for peer in range(n_dp):
        back_rows[peer] = backward[peer * slot_rows : (peer + 1) * slot_rows].astype(bf16)
    swap_start(*back_swap)

    turned[...] = jnp.transpose(features.astype(f32)).astype(bf16)
    own_features = turned[pl.ds(pl.multiple_of(my_mp * width, 16), width), :]
    for head, kept_now in enumerate(kept_back):
        active, second, third, differ, above_bf, inner_bf, first_bf = kept_now
        read_out[head] = dot32(own_features, first_bf)
        act_out[head] = flipped(noisy, first_bf)[:act]
        time_out[:, head, :] = flipped(onehot, first_bf)[:LEVELS]
        inner_out[head] = flipped(active, inner_bf)
        outer_out[head] = flipped(second, above_bf)
        final_out[head] = flipped(differ, third)
    swap_wait(*back_swap)
    arrived = jnp.concatenate([back_in[peer].astype(f32) for peer in range(n_dp)], axis=0)
    arrived = flipped(spread, arrived.astype(bf16))
    for owner in range(n_mp):
        returned[owner] = arrived[owner * slots : (owner + 1) * slots]
    mine = returned[my_mp]
    for sample in range(samples):
        back_out[sample] = mine[READ * sample : READ * (sample + 1)].astype(bf16)

    for unit in range(len(sources)):
        for step in range(half):
            for way, part in legs(step):
                hop(unit, step, way, part).wait_send()
    for offset in range(1, n_dp):
        swap_copy(*small_swap, offset).wait_send()
        swap_copy(*rows_swap, offset).wait_send()
        swap_copy(*back_swap, offset).wait_send()
    for index in range(3):
        for way in range(3):
            for chunk in range(chunks):
                cast_copy(index, way, chunk).wait_send()
    for index in range(2):
        if index == 1:
            sum_near(index).wait_send()
            sum_own(index).wait_send()
        for chunk in range(chunks):
            sum_far(index, chunk).wait_send()
    for offset, who in peers():
        mask_copy(offset, who).wait_send()
        ends_copy(offset, who).wait_send()
        for index in range(2):
            term_copy(index, offset, who).wait_send()


def plan_values():
    anchor = math.cos(0.008 / 1.008 * math.pi / 2) ** 2
    steps = [(level + 1.0) / LEVELS for level in range(LEVELS)]
    return [math.cos((up + 0.008) / 1.008 * math.pi / 2) ** 2 / anchor for up in steps]


def trunk(
    tokens,
    obs_mask,
    norm_gains,
    attn_in,
    attn_out,
    raising,
    lowering,
    embodiment,
    levels,
    actions,
    noise,
    action_dims,
    *head_weights,
):
    n_dp, n_mp = lax.axis_size("dp"), lax.axis_size("mp")
    rows, model = tokens.shape
    samples = obs_mask.shape[0]
    wide = model // 3
    units = 3 * raising.shape[0]
    chunks = rows // CHUNK
    parts = RING_PARTS if raising.shape[1] % (16 * RING_PARTS) == 0 else 1
    slots = samples * READ + (-samples * READ) % 8
    heads = head_weights[0].shape[0]
    bf16, f32 = jnp.bfloat16, jnp.float32
    dma = pltpu.SemaphoreType.DMA
    vmem = pltpu.VMEM
    inner_spec = pl.BlockSpec(memory_space=vmem)
    outer_spec = pl.BlockSpec(memory_space=pl.ANY)
    grads = []
    for index, weight in enumerate(head_weights):
        shape = weight.shape if index else (heads, model // n_mp, weight.shape[2])
        grads.append(jax.ShapeDtypeStruct(shape, f32))
    per_owner = heads * READ
    return pl.pallas_call(
        functools.partial(trunk_kernel, n_dp, n_mp),
        out_shape=[jax.ShapeDtypeStruct((samples, READ, model), bf16)] + grads,
        in_specs=[inner_spec] * 11
        + [pl.BlockSpec(memory_space=pltpu.SMEM)]
        + [outer_spec] * len(head_weights),
        out_specs=[inner_spec] * (1 + len(grads)),
        scratch_shapes=[
            vmem((units, model, model), bf16),
            vmem((3, n_mp, rows, model), bf16),
            vmem((rows, model), f32),
            vmem((n_mp * rows, model), bf16),
            vmem((n_mp * rows, wide), bf16),
            vmem((n_mp, rows, model), bf16),
            vmem((n_mp, rows, model), bf16),
            vmem((2, rows, model), bf16),
            vmem((2, rows, model), bf16),
            vmem((2, rows, model), bf16),
            vmem((2, rows, model), bf16),
            vmem((n_mp,) + obs_mask.shape, jnp.int32),
            vmem((n_mp, slots, model), f32),
            vmem((2, n_mp, n_mp * slots, model), bf16),
            vmem((model, wide), bf16),
            vmem(raising.shape, bf16),
            vmem((n_mp, slots, model), f32),
            dma((units, n_dp, parts)),
            dma((units, n_dp, parts)),
            dma((units,)),
            dma((3, 3, chunks)),
            dma((3, 3, chunks)),
            dma((2, 3, chunks)),
            dma((2, 3, chunks)),
            dma((n_mp,)),
            dma((n_mp,)),
            dma((2, n_mp)),
            dma((2, n_mp)),
            dma((n_mp,)),
            dma((n_mp,)),
        ]
        + [vmem(weight.shape, weight.dtype) for weight in head_weights]
        + [vmem((model, n_dp * per_owner), bf16)]
        + [vmem((n_dp, per_owner, 3 * 128), bf16)] * 2
        + [vmem((n_dp, per_owner, model), bf16)] * 4
        + [dma((len(head_weights),))]
        + [dma((n_dp,))] * 6,
        compiler_params=pltpu.CompilerParams(collective_id=50, has_side_effects=True),
        name="trunk",
    )(
        tokens,
        obs_mask,
        norm_gains,
        attn_in,
        attn_out,
        raising,
        lowering,
        embodiment,
        levels,
        actions,
        noise,
        action_dims,
        *head_weights,
    )


def general_trunk(ident, tokens, obs_mask, norm_gains, attn_in, attn_out, mlp_in, mlp_out, small):
    model = tokens.shape[1]
    width = attn_in.shape[3]
    heads_local = width // HDIM
    samples_local, length = obs_mask.shape
    layer_count = attn_in.shape[0]
    n_mp = lax.axis_size("mp")
    samples_group = samples_local * n_mp
    joined = [
        jnp.concatenate(
            [attn_in[layer, 0], attn_in[layer, 1], attn_in[layer, 2], attn_out[layer].T], axis=1
        )
        for layer in range(layer_count)
    ]
    lowered = [mlp_out[layer].T for layer in range(layer_count)]


    residual = tokens.astype(jnp.float32)
    wide = None
    allowed = None
    mask_group = None
    got_small = None
    position = jnp.arange(length)
    for layer in range(layer_count):
        final = layer == layer_count - 1
        normed = normalize(residual, norm_gains[2 * layer]).astype(jnp.bfloat16)
        if layer == 0:
            sends = [("cast", normed), ("cast", obs_mask), ("swap", small), ("ring", joined[0])]
        else:
            sends = [("cast", normed)]
        if final:
            ends = residual.reshape(samples_local, length, model)[:, length - READ :, :]
            sends += [("cast", ends), ("ring", mlp_in[layer]), ("ring", lowered[layer])]
        got = list(exchange(next(ident), *sends))
        gathered = got.pop(0).reshape(-1, model)
        if layer == 0:
            mask_group = got.pop(0).reshape(samples_group, length)
            got_small = got.pop(0)
            wide = got.pop(0).reshape(model, -1)
            visible = (mask_group == 1) & (position < length - READ)[None, :]
            itself = position[:, None] == position[None, :]
            allowed = visible[:, None, :] | itself[None, :, :]
        if final:
            ends = got.pop(0).reshape(samples_group * READ, model)
            upper = got.pop(0).reshape(model, -1)
            lower = got.pop(0).reshape(model, -1)
            asking = gathered.reshape(samples_group, length, model)[:, length - READ :, :]
            queries = dot32(asking.reshape(-1, model), wide[:, :width]).astype(jnp.bfloat16)
            queries = queries.reshape(samples_group, READ, heads_local, HDIM)
            both = dot32(gathered, wide[:, width : 3 * width]).astype(jnp.bfloat16)
            keys_at = both[:, :width].reshape(samples_group, length, heads_local, HDIM)
            values_at = both[:, width:].reshape(samples_group, length, heads_local, HDIM)
            context = attend(queries, keys_at, values_at, allowed[:, length - READ :, :])
            partial_value = dot_turned(context.reshape(-1, width), wide[:, 3 * width :])
            (terms,) = exchange(next(ident), ("cast", partial_value.astype(jnp.bfloat16)))
            ends = ends + added(terms)
            normed = normalize(ends, norm_gains[2 * layer + 1]).astype(jnp.bfloat16)
            hidden = jax.nn.gelu(dot32(normed, upper), approximate=True).astype(jnp.bfloat16)
            partial_value = dot_turned(hidden, lower)
            (terms,) = exchange(next(ident), ("cast", partial_value.astype(jnp.bfloat16)))
            ends = ends + added(terms)
            break
        projected = dot32(gathered, wide[:, : 3 * width]).astype(jnp.bfloat16)
        split = [
            projected[:, part * width : (part + 1) * width].reshape(
                samples_group, length, heads_local, HDIM
            )
            for part in range(3)
        ]
        context = attend(split[0], split[1], split[2], allowed).reshape(-1, width)
        partial_value = dot_turned(context, wide[:, 3 * width :]).astype(jnp.bfloat16)
        terms, upper = exchange(
            next(ident),
            ("split", partial_value.reshape(n_mp, -1, model)),
            ("ring", mlp_in[layer]),
        )
        residual = residual + added(terms)
        normed = normalize(residual, norm_gains[2 * layer + 1]).astype(jnp.bfloat16)
        gathered, lower = exchange(next(ident), ("cast", normed), ("ring", lowered[layer]))
        raised = dot32(gathered.reshape(-1, model), upper.reshape(model, -1))
        hidden = jax.nn.gelu(raised, approximate=True).astype(jnp.bfloat16)
        partial_value = dot_turned(hidden, lower.reshape(model, -1)).astype(jnp.bfloat16)
        terms, wide = exchange(
            next(ident),
            ("split", partial_value.reshape(n_mp, -1, model)),
            ("ring", joined[layer + 1]),
        )
        wide = wide.reshape(model, -1)
        residual = residual + added(terms)

    return normalize(ends, norm_gains[2 * layer_count]).astype(jnp.bfloat16), got_small


def fused(
    tokens,
    obs_mask,
    norm_gains,
    attn_in,
    attn_out,
    mlp_in,
    mlp_out,
    embodiment,
    levels,
    actions,
    noise,
    action_dims,
    head_read,
    head_act,
    time_table,
    block_in,
    block_out,
    head_out,
):
    outs = trunk(
        tokens,
        obs_mask,
        norm_gains,
        attn_in,
        attn_out,
        mlp_in,
        jnp.swapaxes(mlp_out, 1, 2),
        embodiment.T,
        levels.T,
        actions,
        noise,
        action_dims,
        head_read,
        head_act,
        jnp.swapaxes(time_table, 0, 1),
        block_in,
        block_out,
        jnp.swapaxes(head_out, 1, 2),
    )
    back, read, act, times, inner, outer, final = outs
    return back, read, act, jnp.swapaxes(times, 0, 1), inner, outer, jnp.swapaxes(final, 1, 2)


def fits_fused(tokens, obs_mask, attn_in, mlp_in, head_read, actions):
    n_mp, n_dp = lax.axis_size("mp"), lax.axis_size("dp")
    model, width = tokens.shape[1], attn_in.shape[3]
    pad = model // 3 - width
    return (
        n_mp == 4
        and n_dp % 2 == 0
        and attn_in.shape[0] == 2
        and attn_in.shape[2] % 16 == 0
        and mlp_in.shape[2] == model
        and (model // 3) % 128 == 0
        and 3 * pad == width
        and tokens.shape[0] % CHUNK == 0
        and obs_mask.shape[1] == CHUNK
        and head_read.shape[0] * READ == 8
        and actions.shape[2] <= 128
    )


def on_device(
    tokens,
    obs_mask,
    norm_gains,
    attn_in,
    attn_out,
    mlp_in,
    mlp_out,
    embodiment,
    levels,
    actions,
    noise,
    action_dims,
    head_read,
    head_act,
    time_table,
    block_in,
    block_out,
    head_out,
):
    if fits_fused(tokens, obs_mask, attn_in, mlp_in, head_read, actions):
        return fused(
            tokens,
            obs_mask,
            norm_gains,
            attn_in,
            attn_out,
            mlp_in,
            mlp_out,
            embodiment,
            levels,
            actions,
            noise,
            action_dims,
            head_read,
            head_act,
            time_table,
            block_in,
            block_out,
            head_out,
        )
    model = tokens.shape[1]
    act = actions.shape[2]
    samples_local = obs_mask.shape[0]
    n_mp, n_dp = lax.axis_size("mp"), lax.axis_size("dp")
    my_model, my_owner = lax.axis_index("mp"), lax.axis_index("dp")
    samples_group = samples_local * n_mp
    ident = iter(range(100))

    heads_dev = head_read.shape[0]
    slot_count = heads_dev * n_dp
    owners = embodiment[:, 0]
    table = plan()
    onto = (jnp.arange(slot_count)[:, None] == owners[None, :]).astype(jnp.bfloat16)
    spread_rows = jnp.einsum("es,rq->ersq", onto, jnp.eye(READ, dtype=jnp.bfloat16)).reshape(
        slot_count * READ, samples_group * READ
    )
    small = jnp.concatenate(
        [
            noisy_pair(levels, actions, noise, table),
            noise,
            (levels + 1)[..., None].astype(jnp.bfloat16),
        ],
        axis=-1,
    ).reshape(samples_group * READ, 2 * act + 1)
    small = jnp.pad(small, ((0, 0), (0, -small.shape[1] % 128)))
    small = dot32(spread_rows, small).astype(jnp.bfloat16)
    small = small.reshape(n_dp, heads_dev * READ, small.shape[1])

    readouts, got_small = general_trunk(
        ident, tokens, obs_mask, norm_gains, attn_in, attn_out, mlp_in, mlp_out, small
    )
    send = dot32(spread_rows, readouts).astype(jnp.bfloat16)
    send = send.reshape(n_dp, heads_dev * READ, model)
    (got_features,) = exchange(next(ident), ("swap", send))

    def by_head(values):
        values = values.reshape(n_dp, heads_dev, READ, values.shape[-1])
        return jnp.moveaxis(values, 1, 0).reshape(heads_dev, n_dp * READ, values.shape[-1])

    head_features = by_head(got_features)
    head_small = by_head(got_small)
    head_noisy = head_small[..., :act]
    head_target = head_small[..., act : 2 * act].astype(jnp.float32)
    head_levels = head_small[..., 2 * act].astype(jnp.int32) - 1
    head_onehot = (head_levels[..., None] == jnp.arange(LEVELS)).astype(jnp.bfloat16)
    slot_ids = my_owner * heads_dev + jnp.arange(heads_dev)
    dims_here = jnp.sum(
        jnp.where(jnp.arange(EMB)[None, :] == slot_ids[:, None], action_dims[None, :], 0), axis=1
    )
    column = jnp.arange(act) % ADIM_MAX
    weight_mask = (head_levels >= 0).astype(jnp.float32)[..., None] * (
        column[None, None, :] < dims_here[:, None, None]
    ).astype(jnp.float32)
    others = jnp.einsum("hna,hac->hnc", head_noisy, head_act, preferred_element_type=jnp.float32)
    others = others + jnp.einsum(
        "hnl,hlc->hnc", head_onehot, time_table, preferred_element_type=jnp.float32
    )
    first = (
        jnp.einsum("hnd,hdc->hnc", head_features, head_read, preferred_element_type=jnp.float32)
        + others
    )
    grad_first, grad_inner, grad_outer, grad_final = jax.vmap(head_grads)(
        first,
        block_in.astype(jnp.float32),
        block_out.astype(jnp.float32),
        head_out.astype(jnp.float32),
        head_target,
        weight_mask,
    )
    grad_bf = grad_first.astype(jnp.bfloat16)
    backward = jnp.einsum(
        "hnc,hdc->hnd", grad_bf, head_read, preferred_element_type=jnp.float32
    ).astype(jnp.bfloat16)
    backward = jnp.moveaxis(backward.reshape(heads_dev, n_dp, READ, model), 0, 1)
    (arrived,) = exchange(
        next(ident), ("swap", backward.reshape(n_dp, heads_dev * READ, model))
    )
    mine = lax.dynamic_slice_in_dim(
        spread_rows, my_model * (samples_local * READ), samples_local * READ, 1
    )
    returned = lax.dot_general(
        mine,
        arrived.reshape(slot_count * READ, model),
        (((0,), (0,)), ((), ())),
        preferred_element_type=jnp.float32,
    ).astype(jnp.bfloat16)
    feature_width = model // n_mp
    own_features = lax.dynamic_slice_in_dim(
        head_features, my_model * feature_width, feature_width, 2
    )
    grad_readin = jnp.einsum(
        "hnd,hnc->hdc", own_features, grad_bf, preferred_element_type=jnp.float32
    )
    grad_actin = jnp.einsum("hna,hnc->hac", head_noisy, grad_bf, preferred_element_type=jnp.float32)
    grad_timein = jnp.einsum(
        "hnl,hnc->hlc", head_onehot, grad_bf, preferred_element_type=jnp.float32
    )
    return (
        returned.reshape(samples_local, READ, model),
        grad_readin,
        grad_actin,
        grad_timein,
        grad_inner,
        grad_outer,
        grad_final,
    )


def solution(mesh):
    placed = (
        P(("dp", "mp"), None),
        P(("dp", "mp"), None),
        P(),
        P(None, None, "dp", "mp"),
        P(None, "mp", "dp"),
        P(None, "dp", "mp"),
        P(None, "mp", "dp"),
        P("dp", None),
        P("dp", None),
        P("dp", None, None),
        P("dp", None, None),
        P(),
        P("dp", None, None),
        P("dp", None, None),
        P("dp", None, None),
        P("dp", None, None),
        P("dp", None, None),
        P("dp", None, None),
    )
    return jax.shard_map(
        on_device,
        mesh=mesh,
        in_specs=placed,
        out_specs=(
            P(("dp", "mp"), None, None),
            P("dp", "mp", None),
            P("dp", None, None),
            P("dp", None, None),
            P("dp", None, None),
            P("dp", None, None),
            P("dp", None, None),
        ),
        check_vma=False,
    )
```
